256 devices in a mesh: seq: 32 (over z, y_hi, core), tp: 8 (over y_lo, x).
Axes of the slice: x: 4, y: 4 (y_hi: 2, y_lo: 2; y = y_hi * 2 + y_lo), z: 8, core: 2. Of those that a mesh axis runs over, the one named last changes fastest.
Arguments:
- video_query: bfloat16 [2, 16384, 3072], P(None, 'seq', 'tp'), may hold values from -2048 to 2048
- text_states: bfloat16 [2, 256, 4096], P(None, 'seq'), may hold values from -24 to 24
- key_weight: bfloat16 [4096, 3072], P(None, 'tp'), may hold values from -1 to 1
- value_weight: bfloat16 [4096, 3072], P(None, 'tp'), may hold values from -0.09375 to 0.09375
- text_lengths: int32 [2], replicated, may hold values from 64 to 256, as said below
- output_grad: bfloat16 [2, 16384, 3072], P(None, 'seq', 'tp'), may hold values from -6 to 6
Outputs:
- attended: bfloat16 [2, 16384, 3072], P(None, 'seq', 'tp')
- query_grad: bfloat16 [2, 16384, 3072], P(None, 'seq', 'tp')
- key_weight_grad: float32 [4096, 3072], P('seq', 'tp')
- value_weight_grad: float32 [4096, 3072], P('seq', 'tp')
The draws below stay inside these ranges and needn't reach their ends.
Inputs may be any that keep to these rules, and one draw needn't show every extreme that they name: Keys of sample b at text positions from text_lengths[b] on are masked; one sample has all 256 text tokens.
All inputs are finite; a program needn't handle non-finite values.
Results may differ from the reference program's by a relative error of at most 0.012.
The reference program's roundings to bfloat16 on the way (of `key_states`, `value_states`, `probs_low` and `dscore`) count: a program that leaves them out, or rounds other values in their place, can miss the bound.
Values may be sent and summed in bfloat16 or wider, within the bound.
No kernel may reach another device: no remote copies, remote signals or barrier semaphores. Data moves between devices by JAX's collectives and lax.ppermute only.
A program may use at most 128 MiB of HBM per device.

```python
import math
import jax
import jax.numpy as jnp
from jax import lax

DT = 4096
HEADS = 24
HEAD = 128
TEXT = 256
SAMPLES = 2
VIDEO = 16384


def column_rise(ratio):
    position = jnp.arange(DT, dtype=jnp.float32) / max(DT - 1, 1)
    rising = 1.0 + (ratio - 1.0) * position
    return rising / jnp.sqrt(jnp.mean(rising * rising))


def shared_draw(key):
    text_key = jax.random.fold_in(key, 101)
    weight_key = jax.random.fold_in(key, 102)
    states = jax.random.truncated_normal(text_key, -6.0, 6.0, (SAMPLES, TEXT, DT), jnp.float32)
    states = states * column_rise(3.0)[None, None, :]
    weight = jax.random.truncated_normal(weight_key, -6.0, 6.0, (DT, HEADS * HEAD), jnp.float32) / math.sqrt(DT)
    return (states.astype(jnp.bfloat16), weight.astype(jnp.bfloat16))


def draw_text_states(key, part):
    return shared_draw(key)[0]


def draw_key_weight(key, part):
    return shared_draw(key)[1]


def draw_text_lengths(key, part):
    length_key = jax.random.fold_in(key, 104)
    others = jax.random.randint(jax.random.fold_in(length_key, 1), (SAMPLES,), TEXT // 4, TEXT, jnp.int32)
    chosen = jax.random.randint(jax.random.fold_in(length_key, 2), (), 0, SAMPLES, jnp.int32)
    return jnp.where(jnp.arange(SAMPLES, dtype=jnp.int32) == chosen, jnp.int32(TEXT), others).astype(jnp.int32)


def draw_video_query(key, part):
    query_key = jax.random.fold_in(key, 103)
    feature_count = HEADS * HEAD
    base = jax.random.truncated_normal(query_key, -6.0, 6.0, (SAMPLES, VIDEO, feature_count), jnp.float32)
    return base.astype(jnp.bfloat16)


def steps_of(key, dims, split, smallest, largest):
    factor_of, own = 1.0, jax.random.fold_in(key, 6)
    for dim, blocks in split:
        heights = jnp.exp(jax.random.uniform(jax.random.fold_in(own, dim), (blocks,), jnp.float32, smallest / len(split), largest / len(split)))
        factor_of = factor_of * jnp.repeat(heights, dims[dim] // blocks).reshape([-1 if axis == dim else 1 for axis in range(len(dims))])
    return factor_of


def noise(stream_key, shape, scale, limit, shards=(), held_as=jnp.bfloat16):
    drawn = jax.random.normal(stream_key, shape, jnp.float32) * scale
    if len(shards) > 0:
        drawn = steps_of(stream_key, shape, shards, -0.22, 0.18) * drawn
    return jnp.clip(drawn, min=-limit, max=limit).astype(held_as)


def setup_inputs(seed: int = 0) -> dict:
    key_of = jax.random.split(jax.random.key(seed), 7)
    return {
        "video_query": draw_video_query(jax.random.fold_in(key_of[6], 71), 0),
        "text_states": draw_text_states(jax.random.fold_in(key_of[6], 71), 0),
        "key_weight": draw_key_weight(jax.random.fold_in(key_of[6], 71), 0),
        "value_weight": noise(key_of[3], (DT, HEADS * HEAD), DT ** -0.5, 0.09375, ((1, 8),)),
        "text_lengths": draw_text_lengths(jax.random.fold_in(key_of[6], 71), 0),
        "output_grad": noise(key_of[5], (SAMPLES, VIDEO, HEADS * HEAD), 1.0, 6.0, ((1, 32), (2, 8))),
    }


def reference(video_query, text_states, key_weight, value_weight, text_lengths, output_grad):
    samples = video_query.shape[0]
    key_states = lax.optimization_barrier(jnp.dot(text_states, key_weight, preferred_element_type=jnp.float32).astype(jnp.bfloat16))
    value_states = lax.optimization_barrier(jnp.dot(text_states, value_weight, preferred_element_type=jnp.float32).astype(jnp.bfloat16))
    scaling = 1.0 / math.sqrt(HEAD)
    allowed = jnp.arange(TEXT)[None, None, :] < text_lengths[:, None, None]

    def split_heads(tensor, length):
        return tensor.reshape(samples, length, HEADS, HEAD).transpose(2, 0, 1, 3)

    def per_head(operands):
        query_head, key_head, value_head, grad_head = [piece.astype(jnp.float32) for piece in operands]
        scores = jnp.einsum('bte,ble->btl', query_head, key_head) * scaling
        scores = jnp.where(allowed, scores, -1e+30)
        highest = lax.optimization_barrier(jnp.max(scores, axis=-1, keepdims=True))
        weights = jnp.exp(scores - highest)
        probs = weights / lax.optimization_barrier(jnp.sum(weights, axis=-1, keepdims=True))
        probs_low = lax.optimization_barrier(probs.astype(jnp.bfloat16)).astype(jnp.float32)
        attended = jnp.einsum('btl,ble->bte', probs_low, value_head).astype(jnp.bfloat16)
        dprob = jnp.einsum('bte,ble->btl', grad_head, value_head)
        delta = lax.optimization_barrier(jnp.sum(probs * dprob, axis=-1, keepdims=True))
        dscore = lax.optimization_barrier((probs * (dprob - delta) * scaling).astype(jnp.bfloat16)).astype(jnp.float32)
        query_grad = jnp.einsum('btl,ble->bte', dscore, key_head).astype(jnp.bfloat16)
        key_grad = jnp.einsum('btl,bte->ble', dscore, query_head)
        value_grad = jnp.einsum('btl,bte->ble', probs_low, grad_head)
        return (attended, query_grad, key_grad, value_grad)
    results = lax.map(per_head, (split_heads(video_query, VIDEO), split_heads(key_states, TEXT), split_heads(value_states, TEXT), split_heads(output_grad, VIDEO)))

    def merge_heads(tensor):
        return tensor.transpose(1, 2, 0, 3).reshape(samples, tensor.shape[2], HEADS * HEAD)
    attended = merge_heads(results[0])
    query_grad = merge_heads(results[1])
    key_grad = merge_heads(results[2])
    value_grad = merge_heads(results[3])
    text_wide = text_states.astype(jnp.float32)
    key_raw = jnp.einsum('bld,ble->de', text_wide, key_grad, precision=lax.Precision.HIGHEST)
    value_raw = jnp.einsum('bld,ble->de', text_wide, value_grad, precision=lax.Precision.HIGHEST)
    squares = jnp.sum(key_raw * key_raw) + jnp.sum(value_raw * value_raw)
    spread = jnp.sqrt(squares / (2.0 * DT * HEADS * HEAD) + 1e-06)
    factor = 1.0 / jnp.maximum(spread, 1.0)
    return (attended, query_grad, key_raw * factor, value_raw * factor)
```

```python
import functools
import math

import jax
import jax.numpy as jnp
from jax import lax
from jax.experimental import pallas as pl
from jax.experimental.pallas import tpu as pltpu
from jax.sharding import Mesh
from jax.sharding import PartitionSpec as P

DT = 4096
HEADS = 24
HEAD = 128
ZY = ("z", "yh")
SEQ = ("z", "yh", "core")
TP = ("yl", "x")
ALL = SEQ + TP
SCALING = 1.0 / math.sqrt(HEAD)
BF16 = jnp.bfloat16
F32 = jnp.float32


def dot(a, b, ca, cb):
    return lax.dot_general(a, b, (((ca,), (cb,)), ((), ())), preferred_element_type=F32)


def project_kernel(text_ref, key_ref, value_ref, out_ref):
    groups = out_ref.shape[0]
    features = key_ref.shape[1]
    text = text_ref[...].reshape(-1, DT)
    key = dot(text, key_ref[...], 1, 0).astype(BF16)
    value = dot(text, value_ref[...], 1, 0).astype(BF16)
    both = jnp.concatenate([key, value], axis=-1)
    wide = DT // groups
    for g in range(groups):
        out_ref[g, :, : 2 * features] = both
        out_ref[g, :, 2 * features :] = text[:, g * wide : (g + 1) * wide]


def attend_kernel(lengths_ref, core_ref, query_ref, grad_ref, own_ref, other_ref, attended_ref, query_grad_ref, own_sum_ref, other_sum_ref):
    samples, rows, features = query_ref.shape
    groups = own_ref.shape[0]
    heads = features // HEAD
    core = core_ref[0]
    half = groups * 8
    place = lax.broadcasted_iota(jnp.int32, (2 * half, 1), 0)
    within = place % half
    side = jnp.where(place < half, core, 1 - core)
    token = (within // 8) * 16 + side * 8 + within % 8

    def text_of(b, first):
        cols = slice(first, first + HEAD)
        pieces = [ref[:, b * 8 : (b + 1) * 8, cols].reshape(half, HEAD) for ref in (own_ref, other_ref)]
        return jnp.concatenate(pieces, axis=0)

    def put_sum(value, b, first):
        cols = slice(first, first + HEAD)
        own_sum_ref[:, b * 8 : (b + 1) * 8, cols] = value[:half].reshape(groups, 8, HEAD)
        other_sum_ref[:, b * 8 : (b + 1) * 8, cols] = value[half:].reshape(groups, 8, HEAD).astype(BF16)

    for b in range(samples):
        allowed = token < lengths_ref[b]
        for h in range(heads):
            cols = slice(h * HEAD, (h + 1) * HEAD)
            key = text_of(b, h * HEAD)
            value = text_of(b, features + h * HEAD)
            query = query_ref[b, :, cols]
            grad = grad_ref[b, :, cols]
            scores = dot(key, query, 1, 1) * SCALING
            scores = jnp.where(allowed, scores, -1e30)
            weights = jnp.exp(scores - jnp.max(scores, axis=0, keepdims=True))
            probs = weights * (1.0 / jnp.sum(weights, axis=0, keepdims=True))
            probs_low = probs.astype(BF16)
            dprob = dot(value, grad, 1, 1)
            delta = jnp.sum(probs * dprob, axis=0, keepdims=True)
            dscore = (probs * (dprob - delta) * SCALING).astype(BF16)
            put_sum(dot(dscore, query, 1, 0), b, h * HEAD)
            put_sum(dot(probs_low, grad, 1, 0), b, features + h * HEAD)
            attended_ref[b, :, cols] = dot(probs_low, value, 0, 0).astype(BF16)
            query_grad_ref[b, :, cols] = dot(dscore, key, 0, 0).astype(BF16)


def pair_sum_kernel(own_ref, other_ref, out_ref):
    out_ref[...] = (own_ref[...] + other_ref[...].astype(F32)).astype(BF16)


def total_kernel(parts_ref, out_ref):
    total = parts_ref[0].astype(F32)
    for g in range(1, parts_ref.shape[0]):
        total = total + parts_ref[g].astype(F32)
    total = total.astype(BF16)
    for g in range(out_ref.shape[0]):
        out_ref[g] = total


def weight_kernel(core_ref, own_text_ref, other_text_ref, own_ref, other_ref, raw_ref, square_ref):
    groups, rows, width = own_ref.shape
    first = pl.multiple_of(width + core_ref[0] * HEAD, HEAD)
    raw = None
    for text_ref, sum_ref in ((own_text_ref, own_ref), (other_text_ref, other_ref)):
        text = text_ref[:, :, pl.ds(first, HEAD)].reshape(groups * rows, HEAD)
        part = dot(text, sum_ref[...].reshape(groups * rows, width), 0, 0)
        raw = part if raw is None else raw + part
    raw_ref[...] = raw
    squares = jnp.sum((raw * raw).reshape(-1, 8, width), axis=0)
    lanes = squares[:, :HEAD]
    for at in range(HEAD, width, HEAD):
        lanes = lanes + squares[:, at : at + HEAD]
    square_ref[...] = jnp.sum(lanes, axis=0, keepdims=True)


def call(kernel, out, *args, scalars=0):
    specs = [pl.BlockSpec(memory_space=pltpu.SMEM)] * scalars
    specs += [pl.BlockSpec(memory_space=pltpu.VMEM)] * (len(args) - scalars)
    one = pl.BlockSpec(memory_space=pltpu.VMEM)
    out_specs = one if isinstance(out, jax.ShapeDtypeStruct) else [one] * len(out)
    return pl.pallas_call(kernel, out_shape=out, in_specs=specs, out_specs=out_specs)(*args)


def shape(dims, dtype):
    return jax.ShapeDtypeStruct(dims, dtype)


def swap(array):
    return lax.ppermute(array, "core", [(0, 1), (1, 0)])


def per_device(video_query, text_states, key_weight, value_weight, text_lengths, output_grad):
    samples, video_rows, features = video_query.shape
    text_rows = samples * text_states.shape[1]
    groups = lax.axis_size(ZY)
    wide = 2 * features
    core = lax.axis_index("core").astype(jnp.int32).reshape(1)
    packed = call(project_kernel, shape((groups, text_rows, wide + DT // groups), BF16), text_states, key_weight, value_weight)
    own = lax.all_to_all(packed, ZY, 0, 0, tiled=True)
    other = swap(own)
    like = shape(video_query.shape, BF16)
    block = (groups, text_rows, wide)
    attended, query_grad, own_sum, other_sum = call(
        attend_kernel, [like, like, shape(block, F32), shape(block, BF16)],
        text_lengths, core, video_query, output_grad, own, other, scalars=2,
    )
    pair = call(pair_sum_kernel, shape(block, BF16), own_sum, swap(other_sum))
    parts = lax.all_to_all(pair, ZY, 0, 0, tiled=True)
    own_total = lax.all_to_all(call(total_kernel, shape(block, BF16), parts), ZY, 0, 0, tiled=True)
    other_total = swap(own_total)
    raw, squares = call(
        weight_kernel, [shape((HEAD, wide), F32), shape((1, HEAD), F32)],
        core, own, other, own_total, other_total, scalars=1,
    )
    every = lax.axis_size(ALL)
    local = jnp.sum(squares)
    overall = jnp.sum(lax.all_to_all(jnp.full((every, 1), local), ALL, 0, 0, tiled=True))
    spread = jnp.sqrt(overall / (2.0 * DT * HEADS * HEAD) + 1e-06)
    factor = 1.0 / jnp.maximum(spread, 1.0)
    return (attended, query_grad, raw[:, :features] * factor, raw[:, features:] * factor)


def solution(mesh):
    split = Mesh(mesh.devices.reshape(8, 2, 2, 2, 4), ALL)
    return jax.shard_map(
        per_device,
        mesh=split,
        in_specs=(P(None, SEQ, TP), P(None, SEQ, None), P(None, TP), P(None, TP), P(), P(None, SEQ, TP)),
        out_specs=(P(None, SEQ, TP), P(None, SEQ, TP), P(SEQ, TP), P(SEQ, TP)),
        check_vma=False,
    )
```

```python
import functools
import math

import jax
import jax.numpy as jnp
from jax import lax
from jax.experimental import pallas as pl
from jax.experimental.pallas import tpu as pltpu
from jax.sharding import Mesh
from jax.sharding import PartitionSpec as P

DT = 4096
HEADS = 24
HEAD = 128
CHUNKS = 8
ZY = ("z", "yh")
SEQ = ("z", "yh", "core")
TP = ("yl", "x")
ALL = SEQ + TP
SCALING = 1.0 / math.sqrt(HEAD)
BF16 = jnp.bfloat16
F32 = jnp.float32


def dot(a, b, ca, cb):
    return lax.dot_general(a, b, (((ca,), (cb,)), ((), ())), preferred_element_type=F32)


def project_kernel(text_ref, key_ref, value_ref, out_ref, held_ref, arrived):
    groups = out_ref.shape[0]
    features = key_ref.shape[1]
    step = DT // CHUNKS
    copies = []
    for at in range(CHUNKS):
        rows = pl.ds(at * step, step)
        for which, ref in enumerate((key_ref, value_ref)):
            copy = pltpu.make_async_copy(ref.at[rows], held_ref.at[which, rows], arrived.at[which, at])
            copy.start()
            copies.append(copy)
    text = text_ref[...].reshape(-1, DT)
    sums = [None, None]
    for at in range(CHUNKS):
        rows = slice(at * step, (at + 1) * step)
        for which in range(2):
            copies[2 * at + which].wait()
            part = dot(text[:, rows], held_ref[which, rows], 1, 0)
            sums[which] = part if sums[which] is None else sums[which] + part
    both = jnp.concatenate([total.astype(BF16) for total in sums], axis=-1)
    wide = DT // groups
    for g in range(groups):
        out_ref[g, :, : 2 * features] = both
        out_ref[g, :, 2 * features :] = text[:, g * wide : (g + 1) * wide]


def attend_kernel(lengths_ref, core_ref, query_ref, grad_ref, own_ref, other_ref, attended_ref, query_grad_ref, own_sum_ref, other_sum_ref):
    samples, rows, features = query_ref.shape
    groups = own_ref.shape[0]
    heads = features // HEAD
    core = core_ref[0]
    half = groups * 8
    place = lax.broadcasted_iota(jnp.int32, (2 * half, 1), 0)
    within = place % half
    side = jnp.where(place < half, core, 1 - core)
    token = (within // 8) * 16 + side * 8 + within % 8

    def text_of(b, first):
        cols = slice(first, first + HEAD)
        pieces = [ref[:, b * 8 : (b + 1) * 8, cols].reshape(half, HEAD) for ref in (own_ref, other_ref)]
        return jnp.concatenate(pieces, axis=0)

    def put_sum(value, b, first):
        cols = slice(first, first + HEAD)
        own_sum_ref[:, b * 8 : (b + 1) * 8, cols] = value[:half].reshape(groups, 8, HEAD)
        other_sum_ref[:, b * 8 : (b + 1) * 8, cols] = value[half:].reshape(groups, 8, HEAD).astype(BF16)

    for b in range(samples):
        allowed = token < lengths_ref[b]
        for h in range(heads):
            cols = slice(h * HEAD, (h + 1) * HEAD)
            key = text_of(b, h * HEAD)
            value = text_of(b, features + h * HEAD)
            query = query_ref[b, :, cols]
            grad = grad_ref[b, :, cols]
            scores = dot(key, query, 1, 1) * SCALING
            scores = jnp.where(allowed, scores, -1e30)
            weights = jnp.exp(scores - jnp.max(scores, axis=0, keepdims=True))
            probs = weights * (1.0 / jnp.sum(weights, axis=0, keepdims=True))
            probs_low = probs.astype(BF16)
            dprob = dot(value, grad, 1, 1)
            delta = jnp.sum(probs * dprob, axis=0, keepdims=True)
            dscore = (probs * (dprob - delta) * SCALING).astype(BF16)
            put_sum(dot(dscore, query, 1, 0), b, h * HEAD)
            put_sum(dot(probs_low, grad, 1, 0), b, features + h * HEAD)
            attended_ref[b, :, cols] = dot(probs_low, value, 0, 0).astype(BF16)
            query_grad_ref[b, :, cols] = dot(dscore, key, 0, 0).astype(BF16)


def pair_sum_kernel(own_ref, other_ref, out_ref):
    out_ref[...] = (own_ref[...] + other_ref[...].astype(F32)).astype(BF16)


def total_kernel(parts_ref, out_ref):
    total = parts_ref[0].astype(F32)
    for g in range(1, parts_ref.shape[0]):
        total = total + parts_ref[g].astype(F32)
    total = total.astype(BF16)
    for g in range(out_ref.shape[0]):
        out_ref[g] = total


def weight_kernel(core_ref, own_text_ref, other_text_ref, own_ref, other_ref, raw_ref, square_ref):
    groups, rows, width = own_ref.shape
    first = pl.multiple_of(width + core_ref[0] * HEAD, HEAD)
    raw = None
    for text_ref, sum_ref in ((own_text_ref, own_ref), (other_text_ref, other_ref)):
        text = text_ref[:, :, pl.ds(first, HEAD)].reshape(groups * rows, HEAD)
        part = dot(text, sum_ref[...].reshape(groups * rows, width), 0, 0)
        raw = part if raw is None else raw + part
    raw_ref[...] = raw
    squares = jnp.sum((raw * raw).reshape(-1, 8, width), axis=0)
    lanes = squares[:, :HEAD]
    for at in range(HEAD, width, HEAD):
        lanes = lanes + squares[:, at : at + HEAD]
    square_ref[...] = jnp.sum(lanes, axis=0, keepdims=True)


def call(kernel, out, *args, scalars=0, far=0, scratch=(), mib=12, flops=0):
    specs = [pl.BlockSpec(memory_space=pltpu.SMEM)] * scalars
    specs += [pl.BlockSpec(memory_space=pltpu.VMEM)] * (len(args) - scalars - far)
    specs += [pl.BlockSpec(memory_space=pltpu.HBM)] * far
    one = pl.BlockSpec(memory_space=pltpu.VMEM)
    out_specs = one if isinstance(out, jax.ShapeDtypeStruct) else [one] * len(out)
    return pl.pallas_call(
        kernel, out_shape=out, in_specs=specs, out_specs=out_specs, scratch_shapes=scratch,
        compiler_params=pltpu.CompilerParams(vmem_limit_bytes=mib << 20),
        cost_estimate=pl.CostEstimate(flops=flops, bytes_accessed=0, transcendentals=0) if flops else None,
    )(*args)


def shape(dims, dtype):
    return jax.ShapeDtypeStruct(dims, dtype)


def swap(array):
    return lax.ppermute(array, "core", [(0, 1), (1, 0)])


def per_device(video_query, text_states, key_weight, value_weight, text_lengths, output_grad):
    samples, video_rows, features = video_query.shape
    text_rows = samples * text_states.shape[1]
    groups = lax.axis_size(ZY)
    wide = 2 * features
    core = lax.axis_index("core").astype(jnp.int32).reshape(1)
    packed = call(
        project_kernel, shape((groups, text_rows, wide + DT // groups), BF16), text_states, key_weight, value_weight, far=2, mib=61,
        scratch=[pltpu.VMEM((2, DT, features), BF16), pltpu.SemaphoreType.DMA((2, CHUNKS))],
    )
    own = lax.all_to_all(packed, ZY, 0, 0, tiled=True)
    other = swap(own)
    like = shape(video_query.shape, BF16)
    block = (groups, text_rows, wide)
    attended, query_grad, own_sum, other_sum = call(
        attend_kernel, [like, like, shape(block, F32), shape(block, BF16)],
        text_lengths, core, video_query, output_grad, own, other, scalars=2,
    )
    pair = call(pair_sum_kernel, shape(block, BF16), own_sum, swap(other_sum))
    parts = lax.all_to_all(pair, ZY, 0, 0, tiled=True)
    own_total = lax.all_to_all(call(total_kernel, shape(block, BF16), parts), ZY, 0, 0, tiled=True)
    other_total = swap(own_total)
    raw, squares = call(
        weight_kernel, [shape((HEAD, wide), F32), shape((1, HEAD), F32)],
        core, own, other, own_total, other_total, scalars=1,
    )
    every = lax.axis_size(ALL)
    local = jnp.sum(squares)
    overall = jnp.sum(lax.all_to_all(jnp.full((every, 1), local), ALL, 0, 0, tiled=True))
    spread = jnp.sqrt(overall / (2.0 * DT * HEADS * HEAD) + 1e-06)
    factor = 1.0 / jnp.maximum(spread, 1.0)
    return (attended, query_grad, raw[:, :features] * factor, raw[:, features:] * factor)


def solution(mesh):
    split = Mesh(mesh.devices.reshape(8, 2, 2, 2, 4), ALL)
    return jax.shard_map(
        per_device,
        mesh=split,
        in_specs=(P(None, SEQ, TP), P(None, SEQ, None), P(None, TP), P(None, TP), P(), P(None, SEQ, TP)),
        out_specs=(P(None, SEQ, TP), P(None, SEQ, TP), P(SEQ, TP), P(SEQ, TP)),
        check_vma=False,
    )
```

```python
import functools
import math

import jax
import jax.numpy as jnp
from jax import lax
from jax.experimental import pallas as pl
from jax.experimental.pallas import tpu as pltpu
from jax.sharding import Mesh
from jax.sharding import PartitionSpec as P

DT = 4096
HEADS = 24
HEAD = 128
CHUNKS = 8
ZY = ("z", "yh")
SEQ = ("z", "yh", "core")
TP = ("yl", "x")
ALL = SEQ + TP
SCALING = 1.0 / math.sqrt(HEAD)
BF16 = jnp.bfloat16
F32 = jnp.float32


def dot(a, b, ca, cb):
    return lax.dot_general(a, b, (((ca,), (cb,)), ((), ())), preferred_element_type=F32)


def project_kernel(text_ref, key_ref, value_ref, out_ref, held_ref, arrived):
    groups = out_ref.shape[0]
    features = key_ref.shape[1]
    step = DT // CHUNKS
    copies = []
    for at in range(CHUNKS):
        rows = pl.ds(at * step, step)
        for which, ref in enumerate((key_ref, value_ref)):
            copy = pltpu.make_async_copy(ref.at[rows], held_ref.at[which, rows], arrived.at[which, at])
            copy.start()
            copies.append(copy)
    text = text_ref[...].reshape(-1, DT)
    sums = [None, None]
    for at in range(CHUNKS):
        rows = slice(at * step, (at + 1) * step)
        for which in range(2):
            copies[2 * at + which].wait()
            part = dot(text[:, rows], held_ref[which, rows], 1, 0)
            sums[which] = part if sums[which] is None else sums[which] + part
    both = jnp.concatenate([total.astype(BF16) for total in sums], axis=-1)
    wide = DT // groups
    for g in range(groups):
        out_ref[g, :, : 2 * features] = both
        out_ref[g, :, 2 * features :] = text[:, g * wide : (g + 1) * wide]


def text_of(own_ref, other_ref, b, first):
    half = own_ref.shape[0] * 8
    pieces = [ref[:, b * 8 : (b + 1) * 8, first : first + HEAD].reshape(half, HEAD) for ref in (own_ref, other_ref)]
    return jnp.concatenate(pieces, axis=0)


def score_kernel(lengths_ref, core_ref, query_ref, grad_ref, own_ref, other_ref, own_sum_ref, other_sum_ref, probs_ref, dscore_ref):
    samples, rows, features = query_ref.shape
    groups = own_ref.shape[0]
    heads = features // HEAD
    core = core_ref[0]
    half = groups * 8
    place = lax.broadcasted_iota(jnp.int32, (2 * half, 1), 0)
    within = place % half
    side = jnp.where(place < half, core, 1 - core)
    token = (within // 8) * 16 + side * 8 + within % 8

    def put_sum(value, b, first):
        cols = slice(first, first + HEAD)
        own_sum_ref[:, b * 8 : (b + 1) * 8, cols] = value[:half].reshape(groups, 8, HEAD)
        other_sum_ref[:, b * 8 : (b + 1) * 8, cols] = value[half:].reshape(groups, 8, HEAD).astype(BF16)

    for b in range(samples):
        allowed = token < lengths_ref[b]
        for h in range(heads):
            cols = slice(h * HEAD, (h + 1) * HEAD)
            key = text_of(own_ref, other_ref, b, h * HEAD)
            value = text_of(own_ref, other_ref, b, features + h * HEAD)
            query = query_ref[b, :, cols]
            grad = grad_ref[b, :, cols]
            scores = dot(key, query, 1, 1) * SCALING
            scores = jnp.where(allowed, scores, -1e30)
            weights = jnp.exp(scores - jnp.max(scores, axis=0, keepdims=True))
            probs = weights * (1.0 / jnp.sum(weights, axis=0, keepdims=True))
            probs_low = probs.astype(BF16)
            dprob = dot(value, grad, 1, 1)
            delta = jnp.sum(probs * dprob, axis=0, keepdims=True)
            dscore = (probs * (dprob - delta) * SCALING).astype(BF16)
            put_sum(dot(dscore, query, 1, 0), b, h * HEAD)
            put_sum(dot(probs_low, grad, 1, 0), b, features + h * HEAD)
            probs_ref[b, h] = probs_low
            dscore_ref[b, h] = dscore


def attend_kernel(own_ref, other_ref, probs_ref, dscore_ref, attended_ref, query_grad_ref):
    samples, heads = probs_ref.shape[:2]
    features = heads * HEAD
    for b in range(samples):
        for h in range(heads):
            cols = slice(h * HEAD, (h + 1) * HEAD)
            value = text_of(own_ref, other_ref, b, features + h * HEAD)
            attended_ref[b, :, cols] = dot(probs_ref[b, h], value, 0, 0).astype(BF16)
            key = text_of(own_ref, other_ref, b, h * HEAD)
            query_grad_ref[b, :, cols] = dot(dscore_ref[b, h], key, 0, 0).astype(BF16)


def pair_sum_kernel(own_ref, other_ref, out_ref):
    out_ref[...] = (own_ref[...] + other_ref[...].astype(F32)).astype(BF16)


def total_kernel(parts_ref, out_ref):
    total = parts_ref[0].astype(F32)
    for g in range(1, parts_ref.shape[0]):
        total = total + parts_ref[g].astype(F32)
    total = total.astype(BF16)
    for g in range(out_ref.shape[0]):
        out_ref[g] = total


def weight_kernel(core_ref, own_text_ref, other_text_ref, own_ref, other_ref, raw_ref, square_ref):
    groups, rows, width = own_ref.shape
    first = pl.multiple_of(width + core_ref[0] * HEAD, HEAD)
    raw = None
    for text_ref, sum_ref in ((own_text_ref, own_ref), (other_text_ref, other_ref)):
        text = text_ref[:, :, pl.ds(first, HEAD)].reshape(groups * rows, HEAD)
        part = dot(text, sum_ref[...].reshape(groups * rows, width), 0, 0)
        raw = part if raw is None else raw + part
    raw_ref[...] = raw
    squares = jnp.sum((raw * raw).reshape(-1, 8, width), axis=0)
    lanes = squares[:, :HEAD]
    for at in range(HEAD, width, HEAD):
        lanes = lanes + squares[:, at : at + HEAD]
    square_ref[...] = jnp.broadcast_to(jnp.sum(lanes, keepdims=True), square_ref.shape)


def scale_kernel(raw_ref, squares_ref, key_ref, value_ref):
    overall = jnp.sum(squares_ref[...], keepdims=True)
    spread = jnp.sqrt(overall / (2.0 * DT * HEADS * HEAD) + 1e-06)
    factor = 1.0 / jnp.maximum(spread, 1.0)
    features = key_ref.shape[1]
    key_ref[...] = raw_ref[:, :features] * factor
    value_ref[...] = raw_ref[:, features:] * factor


def call(kernel, out, *args, scalars=0, far=0, scratch=(), mib=12, flops=0):
    specs = [pl.BlockSpec(memory_space=pltpu.SMEM)] * scalars
    specs += [pl.BlockSpec(memory_space=pltpu.VMEM)] * (len(args) - scalars - far)
    specs += [pl.BlockSpec(memory_space=pltpu.HBM)] * far
    one = pl.BlockSpec(memory_space=pltpu.VMEM)
    out_specs = one if isinstance(out, jax.ShapeDtypeStruct) else [one] * len(out)
    return pl.pallas_call(
        kernel, out_shape=out, in_specs=specs, out_specs=out_specs, scratch_shapes=scratch,
        compiler_params=pltpu.CompilerParams(vmem_limit_bytes=mib << 20),
        cost_estimate=pl.CostEstimate(flops=flops, bytes_accessed=0, transcendentals=0) if flops else None,
    )(*args)


def shape(dims, dtype):
    return jax.ShapeDtypeStruct(dims, dtype)


def swap(array):
    return lax.ppermute(array, "core", [(0, 1), (1, 0)])


def per_device(video_query, text_states, key_weight, value_weight, text_lengths, output_grad):
    samples, video_rows, features = video_query.shape
    text_rows = samples * text_states.shape[1]
    groups = lax.axis_size(ZY)
    wide = 2 * features
    core = lax.axis_index("core").astype(jnp.int32).reshape(1)
    packed = call(
        project_kernel, shape((groups, text_rows, wide + DT // groups), BF16), text_states, key_weight, value_weight, far=2, mib=61,
        scratch=[pltpu.VMEM((2, DT, features), BF16), pltpu.SemaphoreType.DMA((2, CHUNKS))],
    )
    own = lax.all_to_all(packed, ZY, 0, 0, tiled=True)
    other = swap(own)
    like = shape(video_query.shape, BF16)
    block = (groups, text_rows, wide)
    tall = shape((samples, features // HEAD, 2 * groups * 8, video_rows), BF16)
    flops = 4 * samples * features * video_rows * 2 * groups * 8
    own_sum, other_sum, probs, dscore = call(
        score_kernel, [shape(block, F32), shape(block, BF16), tall, tall],
        text_lengths, core, video_query, output_grad, own, other, scalars=2, flops=2 * flops,
    )
    attended, query_grad = call(attend_kernel, [like, like], own, other, probs, dscore, flops=flops)
    pair = call(pair_sum_kernel, shape(block, BF16), own_sum, swap(other_sum))
    parts = lax.all_to_all(pair, ZY, 0, 0, tiled=True)
    own_total = lax.all_to_all(call(total_kernel, shape(block, BF16), parts), ZY, 0, 0, tiled=True)
    other_total = swap(own_total)
    every = lax.axis_size(ALL)
    raw, squares = call(
        weight_kernel, [shape((HEAD, wide), F32), shape((every, 1), F32)],
        core, own, other, own_total, other_total, scalars=1,
    )
    squares = lax.all_to_all(squares, ALL, 0, 0, tiled=True)
    weight = shape((HEAD, features), F32)
    key_weight_grad, value_weight_grad = call(scale_kernel, [weight, weight], raw, squares)
    return attended, query_grad, key_weight_grad, value_weight_grad


def solution(mesh):
    split = Mesh(mesh.devices.reshape(8, 2, 2, 2, 4), ALL)
    return jax.shard_map(
        per_device,
        mesh=split,
        in_specs=(P(None, SEQ, TP), P(None, SEQ, None), P(None, TP), P(None, TP), P(), P(None, SEQ, TP)),
        out_specs=(P(None, SEQ, TP), P(None, SEQ, TP), P(SEQ, TP), P(SEQ, TP)),
        check_vma=False,
    )
```

```python
import math

import jax
import jax.numpy as jnp
from jax import lax
from jax.experimental import pallas as pl
from jax.experimental.pallas import tpu as pltpu
from jax.sharding import Mesh
from jax.sharding import PartitionSpec as P


DT = 4096
HEADS = 24
HEAD = 128
CHUNKS = 4
ZY = ("z", "yh")
SEQ = ("z", "yh", "core")
TP = ("yl", "x")
ALL = SEQ + TP
SCALING = 1.0 / math.sqrt(HEAD)
BF16 = jnp.bfloat16
F32 = jnp.float32


def dot(a, b, ca, cb):
    return lax.dot_general(a, b, (((ca,), (cb,)), ((), ())), preferred_element_type=F32)


def project_kernel(text_ref, key_ref, value_ref, out_ref, held_ref, arrived):
    groups = out_ref.shape[0]
    features = key_ref.shape[1]
    step = DT // CHUNKS
    copies = []
    for at in range(CHUNKS):
        rows = pl.ds(at * step, step)
        for which, ref in enumerate((key_ref, value_ref)):
            copy = pltpu.make_async_copy(ref.at[rows], held_ref.at[which, rows], arrived.at[which, at])
            copy.start()
            copies.append(copy)
    text = text_ref[...].reshape(-1, DT)
    wide = DT // groups
    for g in range(groups):
        out_ref[g, :, 2 * features :] = text[:, g * wide : (g + 1) * wide]
    sums = [None, None]
    for at in range(CHUNKS):
        rows = slice(at * step, (at + 1) * step)
        for which in range(2):
            copies[2 * at + which].wait()
            part = dot(text[:, rows], held_ref[which, rows], 1, 0)
            sums[which] = part if sums[which] is None else sums[which] + part
    for which in range(2):
        total = sums[which].astype(BF16)
        for g in range(groups):
            out_ref[g, :, which * features : (which + 1) * features] = total


def text_of(own_ref, other_ref, first_core, b, first):
    half = own_ref.shape[0] * 8
    own, other = [ref[:, b * 8 : (b + 1) * 8, first : first + HEAD].reshape(half, HEAD) for ref in (own_ref, other_ref)]
    return jnp.concatenate([jnp.where(first_core, own, other), jnp.where(first_core, other, own)], axis=0)


def score_kernel(lengths_ref, core_ref, query_ref, grad_ref, own_ref, other_ref, own_sum_ref, other_sum_ref, probs_ref, dscore_ref, columns_ref):
    samples, _, features = query_ref.shape
    groups = own_ref.shape[0]
    heads = features // HEAD
    first_core = core_ref[0] == 0
    half = groups * 8
    place = lax.broadcasted_iota(jnp.int32, (2 * half, 1), 0)
    within = place % half
    token = (within // 8) * 16 + (place // half) * 8 + within % 8
    columns_ref[0] = own_ref[:, :, 2 * features :]
    columns_ref[1] = other_ref[:, :, 2 * features :]

    for b in range(samples):
        allowed = token < lengths_ref[b]
        for h in range(heads):
            cols = slice(h * HEAD, (h + 1) * HEAD)
            key = text_of(own_ref, other_ref, first_core, b, h * HEAD)
            value = text_of(own_ref, other_ref, first_core, b, features + h * HEAD)
            query = query_ref[b, :, cols]
            grad = grad_ref[b, :, cols]
            scores = dot(key, query, 1, 1) * SCALING
            scores = jnp.where(allowed, scores, -1e30)
            weights = jnp.exp(scores - jnp.max(scores, axis=0, keepdims=True))
            probs = weights * (1.0 / jnp.sum(weights, axis=0, keepdims=True))
            probs_low = probs.astype(BF16)
            dprob = dot(value, grad, 1, 1)
            delta = jnp.sum(probs * dprob, axis=0, keepdims=True)
            dscore = (probs * (dprob - delta) * SCALING).astype(BF16)
            key_sum = dot(dscore, query, 1, 0)
            value_sum = dot(probs_low, grad, 1, 0)
            own_sum = jnp.where(first_core, key_sum, value_sum)
            other_sum = jnp.where(first_core, value_sum, key_sum).astype(BF16)
            for side in range(2):
                at = slice(side * 16 + b * 8, side * 16 + (b + 1) * 8)
                from_side = slice(side * half, (side + 1) * half)
                own_sum_ref[:, at, cols] = own_sum[from_side].reshape(groups, 8, HEAD)
                other_sum_ref[:, at, cols] = other_sum[from_side].reshape(groups, 8, HEAD)
            probs_ref[b, h] = probs_low
            dscore_ref[b, h] = dscore


def attend_kernel(core_ref, own_ref, other_ref, probs_ref, dscore_ref, attended_ref, query_grad_ref):
    samples, heads = probs_ref.shape[:2]
    first_core = core_ref[0] == 0
    features = heads * HEAD
    for b in range(samples):
        for h in range(heads):
            cols = slice(h * HEAD, (h + 1) * HEAD)
            value = text_of(own_ref, other_ref, first_core, b, features + h * HEAD)
            attended_ref[b, :, cols] = dot(probs_ref[b, h], value, 0, 0).astype(BF16)
            key = text_of(own_ref, other_ref, first_core, b, h * HEAD)
            query_grad_ref[b, :, cols] = dot(dscore_ref[b, h], key, 0, 0).astype(BF16)


def pair_sum_kernel(own_ref, other_ref, out_ref):
    out_ref[...] = (own_ref[...] + other_ref[...].astype(F32)).astype(BF16)


def total_kernel(parts_ref, out_ref):
    total = parts_ref[0].astype(F32)
    for g in range(1, parts_ref.shape[0]):
        total = total + parts_ref[g].astype(F32)
    total = total.astype(BF16)
    for g in range(out_ref.shape[0]):
        out_ref[g] = total


def weight_kernel(core_ref, columns_ref, total_ref, own_raw_ref, other_raw_ref, square_ref):
    groups, rows, features = total_ref.shape
    half = rows // 2
    core = core_ref[0]
    squares = None
    for raw_ref, feature_core in ((own_raw_ref, core), (other_raw_ref, 1 - core)):
        first = pl.multiple_of(feature_core * HEAD, HEAD)
        raw = None
        for which, side in ((0, core), (1, 1 - core)):
            text = columns_ref[which, :, :, pl.ds(first, HEAD)].reshape(groups * half, HEAD)
            total = total_ref[:, pl.ds(pl.multiple_of(side * half, half), half), :].reshape(groups * half, features)
            part = dot(text, total, 0, 0)
            raw = part if raw is None else raw + part
        raw_ref[...] = raw
        part = jnp.sum((raw * raw).reshape(-1, 8, features), axis=0)
        squares = part if squares is None else squares + part
    lanes = squares[:, :HEAD]
    for at in range(HEAD, features, HEAD):
        lanes = lanes + squares[:, at : at + HEAD]
    square_ref[...] = jnp.broadcast_to(jnp.sum(lanes, keepdims=True), square_ref.shape)


def scale_kernel(core_ref, own_ref, other_ref, squares_ref, key_ref, value_ref):
    overall = jnp.sum(squares_ref[...], keepdims=True)
    spread = jnp.sqrt(overall / (2.0 * DT * HEADS * HEAD) + 1e-06)
    factor = 1.0 / jnp.maximum(spread, 1.0)
    first_core = core_ref[0] == 0
    own = own_ref[...]
    other = other_ref[...]
    key_ref[...] = jnp.where(first_core, own, other) * factor
    value_ref[...] = jnp.where(first_core, other, own) * factor


def call(kernel, out, *args, scalars=0, far=0, scratch=(), mib=12):
    near = pl.BlockSpec(memory_space=pltpu.VMEM)
    specs = [pl.BlockSpec(memory_space=pltpu.SMEM)] * scalars + [near] * (len(args) - scalars - far)
    specs += [pl.BlockSpec(memory_space=pl.ANY)] * far
    return pl.pallas_call(
        kernel, out_shape=out, in_specs=specs, out_specs=near if isinstance(out, jax.ShapeDtypeStruct) else [near] * len(out),
        scratch_shapes=scratch, compiler_params=pltpu.CompilerParams(vmem_limit_bytes=mib << 20),
    )(*args)


def shape(dims, dtype):
    return jax.ShapeDtypeStruct(dims, dtype)


def swap(array):
    return lax.ppermute(array, "core", [(0, 1), (1, 0)])


def exchange(array, axes):
    return lax.all_to_all(array, axes, 0, 0, tiled=True)


def per_device(video_query, text_states, key_weight, value_weight, text_lengths, output_grad):
    samples, video_rows, features = video_query.shape
    text_rows = samples * text_states.shape[1]
    groups = lax.axis_size(ZY)
    wide = 2 * features
    core = lax.axis_index("core").astype(jnp.int32).reshape(1)
    packed = call(
        project_kernel, shape((groups, text_rows, wide + DT // groups), BF16), text_states, key_weight, value_weight, far=2, mib=61,
        scratch=[pltpu.VMEM((2, DT, features), BF16), pltpu.SemaphoreType.DMA((2, CHUNKS))],
    )
    own = exchange(packed, ZY)
    other = swap(own)
    like = shape(video_query.shape, BF16)
    block = (groups, 2 * text_rows, features)
    tall = shape((samples, features // HEAD, 2 * groups * 8, video_rows), BF16)
    own_sum, other_sum, probs, dscore, columns = call(
        score_kernel, [shape(block, F32), shape(block, BF16), tall, tall, shape((2, groups, text_rows, DT // groups), BF16)],
        text_lengths, core, video_query, output_grad, own, other, scalars=2,
    )
    attended, query_grad = call(attend_kernel, [like, like], core, own, other, probs, dscore, scalars=1)
    pair = call(pair_sum_kernel, shape(block, BF16), own_sum, swap(other_sum))
    parts = exchange(pair, ZY)
    totals = exchange(call(total_kernel, shape(block, BF16), parts), ZY)
    every = lax.axis_size(ALL)
    weight = shape((HEAD, features), F32)
    own_raw, other_raw, squares = call(
        weight_kernel, [weight, weight, shape((every, 1), F32)], core, columns, totals, scalars=1,
    )
    squares = exchange(squares, ALL)
    key_weight_grad, value_weight_grad = call(
        scale_kernel, [weight, weight], core, own_raw, swap(other_raw), squares, scalars=1,
    )
    return attended, query_grad, key_weight_grad, value_weight_grad


def solution(mesh):
    split = Mesh(mesh.devices.reshape(8, 2, 2, 2, 4), ALL)
    return jax.shard_map(
        per_device,
        mesh=split,
        in_specs=(P(None, SEQ, TP), P(None, SEQ, None), P(None, TP), P(None, TP), P(), P(None, SEQ, TP)),
        out_specs=(P(None, SEQ, TP), P(None, SEQ, TP), P(SEQ, TP), P(SEQ, TP)),
        check_vma=False,
    )
```

```python
import math

import jax
import jax.numpy as jnp
from jax import lax
from jax.experimental import pallas as pl
from jax.experimental.pallas import tpu as pltpu
from jax.sharding import Mesh
from jax.sharding import PartitionSpec as P


DT = 4096
HEADS = 24
HEAD = 128
CHUNKS = 4
ZY = ("z", "yh")
SEQ = ("z", "yh", "core")
TP = ("yl", "x")
ALL = SEQ + TP
SCALING = 1.0 / math.sqrt(HEAD)
BF16 = jnp.bfloat16
F32 = jnp.float32


def dot(a, b, ca, cb):
    return lax.dot_general(a, b, (((ca,), (cb,)), ((), ())), preferred_element_type=F32)


def project_kernel(text_ref, key_ref, value_ref, out_ref, states_ref, held_ref, arrived, here):
    groups = out_ref.shape[0]
    features = key_ref.shape[1]
    step = DT // CHUNKS
    states = pltpu.make_async_copy(text_ref, states_ref, here)
    states.start()
    copies = []
    for at in range(CHUNKS):
        rows = pl.ds(at * step, step)
        for which, ref in enumerate((key_ref, value_ref)):
            copy = pltpu.make_async_copy(ref.at[rows], held_ref.at[which, rows], arrived.at[which, at])
            copy.start()
            copies.append(copy)
    states.wait()
    text = states_ref[...].reshape(-1, DT)
    wide = DT // groups
    for g in range(groups):
        out_ref[g, :, 2 * features :] = text[:, g * wide : (g + 1) * wide]
    sums = [None, None]
    for at in range(CHUNKS):
        rows = slice(at * step, (at + 1) * step)
        for which in range(2):
            copies[2 * at + which].wait()
            part = dot(text[:, rows], held_ref[which, rows], 1, 0)
            sums[which] = part if sums[which] is None else sums[which] + part
    for which in range(2):
        total = sums[which].astype(BF16)
        for g in range(groups):
            out_ref[g, :, which * features : (which + 1) * features] = total


def text_of(own_ref, other_ref, first_core, b, first):
    half = own_ref.shape[0] * 8
    own, other = [ref[:, b * 8 : (b + 1) * 8, first : first + HEAD].reshape(half, HEAD) for ref in (own_ref, other_ref)]
    return jnp.concatenate([jnp.where(first_core, own, other), jnp.where(first_core, other, own)], axis=0)


def score_kernel(lengths_ref, core_ref, query_ref, grad_ref, own_ref, other_ref, own_sum_ref, other_sum_ref, probs_ref, dscore_ref, columns_ref):
    samples, _, features = query_ref.shape
    groups = own_ref.shape[0]
    heads = features // HEAD
    first_core = core_ref[0] == 0
    half = groups * 8
    place = lax.broadcasted_iota(jnp.int32, (2 * half, 1), 0)
    within = place % half
    token = (within // 8) * 16 + (place // half) * 8 + within % 8
    columns_ref[0] = own_ref[:, :, 2 * features :]
    columns_ref[1] = other_ref[:, :, 2 * features :]

    def products(b, h):
        cols = slice(h * HEAD, (h + 1) * HEAD)
        key = text_of(own_ref, other_ref, first_core, b, h * HEAD)
        value = text_of(own_ref, other_ref, first_core, b, features + h * HEAD)
        return dot(key, query_ref[b, :, cols], 1, 1), dot(value, grad_ref[b, :, cols], 1, 1)

    def weigh(b, h, scores, dprob):
        scores = jnp.where(token < lengths_ref[b], scores * SCALING, -1e30)
        weights = jnp.exp(scores - jnp.max(scores, axis=0, keepdims=True))
        probs = weights * (1.0 / jnp.sum(weights, axis=0, keepdims=True))
        probs_low = probs.astype(BF16)
        delta = jnp.sum(probs * dprob, axis=0, keepdims=True)
        dscore = (probs * (dprob - delta) * SCALING).astype(BF16)
        probs_ref[b, h] = probs_low
        dscore_ref[b, h] = dscore
        return b, h, probs_low, dscore

    def add_up(b, h, probs_low, dscore):
        cols = slice(h * HEAD, (h + 1) * HEAD)
        key_sum = dot(dscore, query_ref[b, :, cols], 1, 0)
        value_sum = dot(probs_low, grad_ref[b, :, cols], 1, 0)
        own_sum = jnp.where(first_core, key_sum, value_sum)
        other_sum = jnp.where(first_core, value_sum, key_sum).astype(BF16)
        for side in range(2):
            at = slice(side * 16 + b * 8, side * 16 + (b + 1) * 8)
            from_side = slice(side * half, (side + 1) * half)
            own_sum_ref[:, at, cols] = own_sum[from_side].reshape(groups, 8, HEAD)
            other_sum_ref[:, at, cols] = other_sum[from_side].reshape(groups, 8, HEAD)

    jobs = [(b, h) for b in range(samples) for h in range(heads)]
    ahead = products(*jobs[0])
    behind = None
    for at, job in enumerate(jobs):
        now = ahead
        if at + 1 < len(jobs):
            ahead = products(*jobs[at + 1])
        if behind is not None:
            add_up(*behind)
        behind = weigh(*job, *now)
    add_up(*behind)


def attend_kernel(core_ref, own_ref, other_ref, probs_ref, dscore_ref, attended_ref, query_grad_ref, held_ref, sent):
    samples, heads = probs_ref.shape[:2]
    first_core = core_ref[0] == 0
    features = heads * HEAD
    copies = []
    for b in range(samples):
        for h in range(heads):
            cols = slice(h * HEAD, (h + 1) * HEAD)
            value = text_of(own_ref, other_ref, first_core, b, features + h * HEAD)
            held_ref[0, b, :, cols] = dot(probs_ref[b, h], value, 0, 0).astype(BF16)
            key = text_of(own_ref, other_ref, first_core, b, h * HEAD)
            held_ref[1, b, :, cols] = dot(dscore_ref[b, h], key, 0, 0).astype(BF16)
        for which, ref in enumerate((attended_ref, query_grad_ref)):
            copy = pltpu.make_async_copy(held_ref.at[which, b], ref.at[b], sent.at[which, b])
            copy.start()
            copies.append(copy)
    for copy in copies:
        copy.wait()


def pair_sum_kernel(own_ref, other_ref, out_ref):
    out_ref[...] = (own_ref[...] + other_ref[...].astype(F32)).astype(BF16)


def total_kernel(parts_ref, out_ref):
    total = parts_ref[0].astype(F32)
    for g in range(1, parts_ref.shape[0]):
        total = total + parts_ref[g].astype(F32)
    total = total.astype(BF16)
    for g in range(out_ref.shape[0]):
        out_ref[g] = total


def weight_kernel(core_ref, columns_ref, total_ref, own_raw_ref, other_raw_ref, square_ref):
    groups, rows, features = total_ref.shape
    half = rows // 2
    core = core_ref[0]
    squares = None
    for raw_ref, feature_core in ((own_raw_ref, core), (other_raw_ref, 1 - core)):
        first = pl.multiple_of(feature_core * HEAD, HEAD)
        raw = None
        for which, side in ((0, core), (1, 1 - core)):
            text = columns_ref[which, :, :, pl.ds(first, HEAD)].reshape(groups * half, HEAD)
            total = total_ref[:, pl.ds(pl.multiple_of(side * half, half), half), :].reshape(groups * half, features)
            part = dot(text, total, 0, 0)
            raw = part if raw is None else raw + part
        raw_ref[...] = raw
        part = jnp.sum((raw * raw).reshape(-1, 8, features), axis=0)
        squares = part if squares is None else squares + part
    lanes = squares[:, :HEAD]
    for at in range(HEAD, features, HEAD):
        lanes = lanes + squares[:, at : at + HEAD]
    square_ref[...] = jnp.broadcast_to(jnp.sum(lanes, keepdims=True), square_ref.shape)


def scale_kernel(core_ref, own_ref, other_ref, squares_ref, key_ref, value_ref):
    overall = jnp.sum(squares_ref[...], keepdims=True)
    spread = jnp.sqrt(overall / (2.0 * DT * HEADS * HEAD) + 1e-06)
    factor = 1.0 / jnp.maximum(spread, 1.0)
    first_core = core_ref[0] == 0
    own = own_ref[...]
    other = other_ref[...]
    key_ref[...] = jnp.where(first_core, own, other) * factor
    value_ref[...] = jnp.where(first_core, other, own) * factor


def call(kernel, out, *args, scalars=0, far=0, far_out=False, scratch=(), mib=12):
    near, away = [pl.BlockSpec(memory_space=space) for space in (pltpu.VMEM, pl.ANY)]
    specs = [pl.BlockSpec(memory_space=pltpu.SMEM)] * scalars + [near] * (len(args) - scalars - far) + [away] * far
    out_spec = away if far_out else near
    return pl.pallas_call(
        kernel, out_shape=out, in_specs=specs, out_specs=out_spec if isinstance(out, jax.ShapeDtypeStruct) else [out_spec] * len(out),
        scratch_shapes=scratch, compiler_params=pltpu.CompilerParams(vmem_limit_bytes=int(mib * 1048576)),
    )(*args)


def shape(dims, dtype):
    return jax.ShapeDtypeStruct(dims, dtype)


def swap(array):
    return lax.ppermute(array, "core", [(0, 1), (1, 0)])


def exchange(array, axes):
    return lax.all_to_all(array, axes, 0, 0, tiled=True)


def per_device(video_query, text_states, key_weight, value_weight, text_lengths, output_grad):
    samples, video_rows, features = video_query.shape
    text_rows = samples * text_states.shape[1]
    groups = lax.axis_size(ZY)
    wide = 2 * features
    core = lax.axis_index("core").astype(jnp.int32).reshape(1)
    packed = call(
        project_kernel, shape((groups, text_rows, wide + DT // groups), BF16), text_states, key_weight, value_weight, far=3, mib=61,
        scratch=[
            pltpu.VMEM(text_states.shape, BF16), pltpu.VMEM((2, DT, features), BF16),
            pltpu.SemaphoreType.DMA((2, CHUNKS)), pltpu.SemaphoreType.DMA,
        ],
    )
    own = exchange(packed, ZY)
    other = swap(own)
    like = shape(video_query.shape, BF16)
    block = (groups, 2 * text_rows, features)
    tall = shape((samples, features // HEAD, 2 * groups * 8, video_rows), BF16)
    own_sum, other_sum, probs, dscore, columns = call(
        score_kernel, [shape(block, F32), shape(block, BF16), tall, tall, shape((2, groups, text_rows, DT // groups), BF16)],
        text_lengths, core, video_query, output_grad, own, other, scalars=2,
    )
    attended, query_grad = call(
        attend_kernel, [like, like], core, own, other, probs, dscore, scalars=1, far_out=True,
        scratch=[pltpu.VMEM((2,) + video_query.shape, BF16), pltpu.SemaphoreType.DMA((2, samples))],
    )
    pair = call(pair_sum_kernel, shape(block, BF16), own_sum, swap(other_sum))
    parts = exchange(pair, ZY)
    totals = exchange(call(total_kernel, shape(block, BF16), parts), ZY)
    every = lax.axis_size(ALL)
    weight = shape((HEAD, features), F32)
    own_raw, other_raw, squares = call(
        weight_kernel, [weight, weight, shape((every, 1), F32)], core, columns, totals, scalars=1,
    )
    squares = exchange(squares, ALL)
    key_weight_grad, value_weight_grad = call(
        scale_kernel, [weight, weight], core, own_raw, swap(other_raw), squares, scalars=1,
    )
    return attended, query_grad, key_weight_grad, value_weight_grad


def solution(mesh):
    split = Mesh(mesh.devices.reshape(8, 2, 2, 2, 4), ALL)
    return jax.shard_map(
        per_device,
        mesh=split,
        in_specs=(P(None, SEQ, TP), P(None, SEQ, None), P(None, TP), P(None, TP), P(), P(None, SEQ, TP)),
        out_specs=(P(None, SEQ, TP), P(None, SEQ, TP), P(SEQ, TP), P(SEQ, TP)),
        check_vma=False,
    )
```

```python
import math

import jax
import jax.numpy as jnp
from jax import lax
from jax.experimental import pallas as pl
from jax.experimental.pallas import tpu as pltpu
from jax.sharding import Mesh
from jax.sharding import PartitionSpec as P


DT = 4096
HEADS = 24
HEAD = 128
CHUNKS = 4
ZY = ("z", "yh")
SEQ = ("z", "yh", "core")
TP = ("yl", "x")
ALL = SEQ + TP
ONE_CORE = ZY + TP
SCALING = 1.0 / math.sqrt(HEAD)
BF16 = jnp.bfloat16
F32 = jnp.float32


def dot(a, b, ca, cb):
    return lax.dot_general(a, b, (((ca,), (cb,)), ((), ())), preferred_element_type=F32)


def project_kernel(text_ref, key_ref, value_ref, out_ref, states_ref, held_ref, arrived, here):
    groups = out_ref.shape[0]
    features = key_ref.shape[1]
    step = DT // CHUNKS
    states = pltpu.make_async_copy(text_ref, states_ref, here)
    states.start()
    copies = []
    for at in range(CHUNKS):
        rows = pl.ds(at * step, step)
        for which, ref in enumerate((key_ref, value_ref)):
            copy = pltpu.make_async_copy(ref.at[rows], held_ref.at[which, rows], arrived.at[which, at])
            copy.start()
            copies.append(copy)
    states.wait()
    text = states_ref[...].reshape(-1, DT)
    wide = DT // groups
    for g in range(groups):
        out_ref[g, :, 2 * features :] = text[:, g * wide : (g + 1) * wide]
    sums = [None, None]
    for at in range(CHUNKS):
        rows = slice(at * step, (at + 1) * step)
        for which in range(2):
            copies[2 * at + which].wait()
            part = dot(text[:, rows], held_ref[which, rows], 1, 0)
            sums[which] = part if sums[which] is None else sums[which] + part
    for which in range(2):
        total = sums[which].astype(BF16)
        for g in range(groups):
            out_ref[g, :, which * features : (which + 1) * features] = total


def text_of(own_ref, other_ref, first_core, b, first):
    half = own_ref.shape[0] * 8
    own, other = [ref[:, b * 8 : (b + 1) * 8, first : first + HEAD].reshape(half, HEAD) for ref in (own_ref, other_ref)]
    return jnp.concatenate([jnp.where(first_core, own, other), jnp.where(first_core, other, own)], axis=0)


def score_kernel(lengths_ref, core_ref, query_ref, grad_ref, own_ref, other_ref, own_sum_ref, other_sum_ref, probs_ref, dscore_ref, columns_ref):
    samples, _, features = query_ref.shape
    groups = own_ref.shape[0]
    heads = features // HEAD
    first_core = core_ref[0] == 0
    half = groups * 8
    place = lax.broadcasted_iota(jnp.int32, (2 * half, 1), 0)
    within = place % half
    token = (within // 8) * 16 + (place // half) * 8 + within % 8
    columns_ref[0] = own_ref[:, :, 2 * features :]
    columns_ref[1] = other_ref[:, :, 2 * features :]

    def products(b, h):
        cols = slice(h * HEAD, (h + 1) * HEAD)
        key = text_of(own_ref, other_ref, first_core, b, h * HEAD)
        value = text_of(own_ref, other_ref, first_core, b, features + h * HEAD)
        return dot(key, query_ref[b, :, cols], 1, 1), dot(value, grad_ref[b, :, cols], 1, 1)

    def weigh(b, h, scores, dprob):
        scores = jnp.where(token < lengths_ref[b], scores * SCALING, -1e30)
        weights = jnp.exp(scores - jnp.max(scores, axis=0, keepdims=True))
        probs = weights * (1.0 / jnp.sum(weights, axis=0, keepdims=True))
        probs_low = probs.astype(BF16)
        delta = jnp.sum(probs * dprob, axis=0, keepdims=True)
        dscore = (probs * (dprob - delta) * SCALING).astype(BF16)
        probs_ref[b, h] = probs_low
        dscore_ref[b, h] = dscore
        return b, h, probs_low, dscore

    def add_up(b, h, probs_low, dscore):
        cols = slice(h * HEAD, (h + 1) * HEAD)
        key_sum = dot(dscore, query_ref[b, :, cols], 1, 0)
        value_sum = dot(probs_low, grad_ref[b, :, cols], 1, 0)
        own_sum = jnp.where(first_core, key_sum, value_sum)
        other_sum = jnp.where(first_core, value_sum, key_sum).astype(BF16)
        for side in range(2):
            at = slice(side * 16 + b * 8, side * 16 + (b + 1) * 8)
            from_side = slice(side * half, (side + 1) * half)
            own_sum_ref[:, at, cols] = own_sum[from_side].reshape(groups, 8, HEAD)
            other_sum_ref[:, at, cols] = other_sum[from_side].reshape(groups, 8, HEAD)

    jobs = [(b, h) for b in range(samples) for h in range(heads)]
    ahead = products(*jobs[0])
    behind = None
    for at, job in enumerate(jobs):
        now = ahead
        if at + 1 < len(jobs):
            ahead = products(*jobs[at + 1])
        if behind is not None:
            add_up(*behind)
        behind = weigh(*job, *now)
    add_up(*behind)


def attend_kernel(core_ref, own_ref, other_ref, probs_ref, dscore_ref, attended_ref, query_grad_ref, held_ref, sent):
    samples, heads = probs_ref.shape[:2]
    first_core = core_ref[0] == 0
    features = heads * HEAD
    copies = []
    for b in range(samples):
        for h in range(heads):
            cols = slice(h * HEAD, (h + 1) * HEAD)
            value = text_of(own_ref, other_ref, first_core, b, features + h * HEAD)
            held_ref[0, b, :, cols] = dot(probs_ref[b, h], value, 0, 0).astype(BF16)
            key = text_of(own_ref, other_ref, first_core, b, h * HEAD)
            held_ref[1, b, :, cols] = dot(dscore_ref[b, h], key, 0, 0).astype(BF16)
        for which, ref in enumerate((attended_ref, query_grad_ref)):
            copy = pltpu.make_async_copy(held_ref.at[which, b], ref.at[b], sent.at[which, b])
            copy.start()
            copies.append(copy)
    for copy in copies:
        copy.wait()


def pair_sum_kernel(own_ref, other_ref, out_ref):
    out_ref[...] = (own_ref[...] + other_ref[...].astype(F32)).astype(BF16)


def total_kernel(parts_ref, out_ref):
    total = parts_ref[0].astype(F32)
    for g in range(1, parts_ref.shape[0]):
        total = total + parts_ref[g].astype(F32)
    total = total.astype(BF16)
    for g in range(out_ref.shape[0]):
        out_ref[g] = total


def weight_kernel(core_ref, columns_ref, total_ref, own_raw_ref, other_raw_ref, square_ref):
    groups, rows, features = total_ref.shape
    half = rows // 2
    core = core_ref[0]
    squares = None
    for raw_ref, feature_core in ((own_raw_ref, core), (other_raw_ref, 1 - core)):
        first = pl.multiple_of(feature_core * HEAD, HEAD)
        raw = None
        for which, side in ((0, core), (1, 1 - core)):
            text = columns_ref[which, :, :, pl.ds(first, HEAD)].reshape(groups * half, HEAD)
            total = total_ref[:, pl.ds(pl.multiple_of(side * half, half), half), :].reshape(groups * half, features)
            part = dot(text, total, 0, 0)
            raw = part if raw is None else raw + part
        raw_ref[...] = raw
        part = jnp.sum((raw * raw).reshape(-1, 8, features), axis=0)
        squares = part if squares is None else squares + part
    lanes = squares[:, :HEAD]
    for at in range(HEAD, features, HEAD):
        lanes = lanes + squares[:, at : at + HEAD]
    square_ref[...] = jnp.broadcast_to(jnp.sum(lanes, keepdims=True), square_ref.shape)


def scale_kernel(core_ref, own_ref, other_ref, own_squares_ref, other_squares_ref, key_ref, value_ref):
    overall = jnp.sum(own_squares_ref[...] + other_squares_ref[...], keepdims=True)
    spread = jnp.sqrt(overall / (2.0 * DT * HEADS * HEAD) + 1e-06)
    factor = 1.0 / jnp.maximum(spread, 1.0)
    first_core = core_ref[0] == 0
    own = own_ref[...]
    other = other_ref[...]
    key_ref[...] = jnp.where(first_core, own, other) * factor
    value_ref[...] = jnp.where(first_core, other, own) * factor


def call(kernel, out, *args, scalars=0, far=0, far_out=False, scratch=(), mib=12):
    near, away = [pl.BlockSpec(memory_space=space) for space in (pltpu.VMEM, pl.ANY)]
    specs = [pl.BlockSpec(memory_space=pltpu.SMEM)] * scalars + [near] * (len(args) - scalars - far) + [away] * far
    out_spec = away if far_out else near
    return pl.pallas_call(
        kernel, out_shape=out, in_specs=specs, out_specs=out_spec if isinstance(out, jax.ShapeDtypeStruct) else [out_spec] * len(out),
        scratch_shapes=scratch, compiler_params=pltpu.CompilerParams(vmem_limit_bytes=int(mib * 1048576)),
    )(*args)


def shape(dims, dtype):
    return jax.ShapeDtypeStruct(dims, dtype)


def swap(array):
    return lax.ppermute(array, "core", [(0, 1), (1, 0)])


def exchange(array, axes):
    return lax.all_to_all(array, axes, 0, 0, tiled=True)


def per_device(video_query, text_states, key_weight, value_weight, text_lengths, output_grad):
    samples, video_rows, features = video_query.shape
    text_rows = samples * text_states.shape[1]
    groups = lax.axis_size(ZY)
    wide = 2 * features
    core = lax.axis_index("core").astype(jnp.int32).reshape(1)
    packed = call(
        project_kernel, shape((groups, text_rows, wide + DT // groups), BF16), text_states, key_weight, value_weight, far=3, mib=61,
        scratch=[
            pltpu.VMEM(text_states.shape, BF16), pltpu.VMEM((2, DT, features), BF16),
            pltpu.SemaphoreType.DMA((2, CHUNKS)), pltpu.SemaphoreType.DMA,
        ],
    )
    own = exchange(packed, ZY)
    other = swap(own)
    like = shape(video_query.shape, BF16)
    block = (groups, 2 * text_rows, features)
    tall = shape((samples, features // HEAD, 2 * groups * 8, video_rows), BF16)
    own_sum, other_sum, probs, dscore, columns = call(
        score_kernel, [shape(block, F32), shape(block, BF16), tall, tall, shape((2, groups, text_rows, DT // groups), BF16)],
        text_lengths, core, video_query, output_grad, own, other, scalars=2,
    )
    attended, query_grad = call(
        attend_kernel, [like, like], core, own, other, probs, dscore, scalars=1, far_out=True,
        scratch=[pltpu.VMEM((2,) + video_query.shape, BF16), pltpu.SemaphoreType.DMA((2, samples))],
    )
    pair = call(pair_sum_kernel, shape(block, BF16), own_sum, swap(other_sum))
    parts = exchange(pair, ZY)
    totals = exchange(call(total_kernel, shape(block, BF16), parts), ZY)
    every = lax.axis_size(ONE_CORE)
    weight = shape((HEAD, features), F32)
    own_raw, other_raw, squares = call(
        weight_kernel, [weight, weight, shape((every, 1), F32)], core, columns, totals, scalars=1,
    )
    squares = exchange(squares, ONE_CORE)
    key_weight_grad, value_weight_grad = call(
        scale_kernel, [weight, weight], core, own_raw, swap(other_raw), squares, swap(squares), scalars=1,
    )
    return attended, query_grad, key_weight_grad, value_weight_grad


def solution(mesh):
    split = Mesh(mesh.devices.reshape(8, 2, 2, 2, 4), ALL)
    return jax.shard_map(
        per_device,
        mesh=split,
        in_specs=(P(None, SEQ, TP), P(None, SEQ, None), P(None, TP), P(None, TP), P(), P(None, SEQ, TP)),
        out_specs=(P(None, SEQ, TP), P(None, SEQ, TP), P(SEQ, TP), P(SEQ, TP)),
        check_vma=False,
    )
```

```python
import math

import jax
import jax.numpy as jnp
from jax import lax
from jax.experimental import pallas as pl
from jax.experimental.pallas import tpu as pltpu
from jax.sharding import Mesh
from jax.sharding import PartitionSpec as P


DT = 4096
HEADS = 24
HEAD = 128
CHUNKS = 2
ZY = ("z", "yh")
SEQ = ("z", "yh", "core")
TP = ("yl", "x")
ALL = SEQ + TP
SCALING = 1.0 / math.sqrt(HEAD)
BF16 = jnp.bfloat16
F32 = jnp.float32


def dot(a, b, ca, cb):
    return lax.dot_general(a, b, (((ca,), (cb,)), ((), ())), preferred_element_type=F32)


def project_kernel(text_ref, key_ref, value_ref, out_ref, states_ref, held_ref, arrived, here):
    groups = out_ref.shape[0]
    features = key_ref.shape[1]
    step = DT // CHUNKS
    states = pltpu.make_async_copy(text_ref, states_ref, here)
    states.start()
    copies = []
    for at in range(CHUNKS):
        rows = pl.ds(at * step, step)
        for which, ref in enumerate((key_ref, value_ref)):
            copy = pltpu.make_async_copy(ref.at[rows], held_ref.at[rows, pl.ds(which * features, features)], arrived.at[which, at])
            copy.start()
            copies.append(copy)
    states.wait()
    text = states_ref[...].reshape(-1, DT)
    wide = DT // groups
    for g in range(groups):
        out_ref[g, :, 2 * features :] = text[:, g * wide : (g + 1) * wide]
    total = None
    for at in range(CHUNKS):
        rows = slice(at * step, (at + 1) * step)
        copies[2 * at].wait()
        copies[2 * at + 1].wait()
        part = dot(text[:, rows], held_ref[rows], 1, 0)
        total = part if total is None else total + part
    total = total.astype(BF16)
    for g in range(groups):
        out_ref[g, :, : 2 * features] = total


def text_of(own_ref, other_ref, first_core, b, first):
    half = own_ref.shape[0] * 8
    own, other = [ref[:, b * 8 : (b + 1) * 8, first : first + HEAD].reshape(half, HEAD) for ref in (own_ref, other_ref)]
    return jnp.concatenate([jnp.where(first_core, own, other), jnp.where(first_core, other, own)], axis=0)


def score_kernel(lengths_ref, core_ref, query_ref, grad_ref, own_ref, other_ref, own_sum_ref, other_sum_ref, probs_ref, dscore_ref, columns_ref):
    samples, _, features = query_ref.shape
    groups = own_ref.shape[0]
    heads = features // HEAD
    first_core = core_ref[0] == 0
    half = groups * 8
    place = lax.broadcasted_iota(jnp.int32, (2 * half, 1), 0)
    within = place % half
    token = (within // 8) * 16 + (place // half) * 8 + within % 8
    columns_ref[0] = own_ref[:, :, 2 * features :]
    columns_ref[1] = other_ref[:, :, 2 * features :]

    def products(b, h):
        cols = slice(h * HEAD, (h + 1) * HEAD)
        key = text_of(own_ref, other_ref, first_core, b, h * HEAD)
        value = text_of(own_ref, other_ref, first_core, b, features + h * HEAD)
        return dot(key, query_ref[b, :, cols], 1, 1), dot(value, grad_ref[b, :, cols], 1, 1)

    def weigh(b, h, scores, dprob):
        scores = jnp.where(token < lengths_ref[b], scores * SCALING, -1e30)
        weights = jnp.exp(scores - jnp.max(scores, axis=0, keepdims=True))
        probs = weights * (1.0 / jnp.sum(weights, axis=0, keepdims=True))
        probs_low = probs.astype(BF16)
        delta = jnp.sum(probs * dprob, axis=0, keepdims=True)
        dscore = (probs * (dprob - delta) * SCALING).astype(BF16)
        probs_ref[b, h] = probs_low
        dscore_ref[b, h] = dscore
        return b, h, probs_low, dscore

    def add_up(b, h, probs_low, dscore):
        cols = slice(h * HEAD, (h + 1) * HEAD)
        key_sum = dot(dscore, query_ref[b, :, cols], 1, 0)
        value_sum = dot(probs_low, grad_ref[b, :, cols], 1, 0)
        own_sum = jnp.where(first_core, key_sum, value_sum)
        other_sum = jnp.where(first_core, value_sum, key_sum).astype(BF16)
        for side in range(2):
            at = slice(side * 16 + b * 8, side * 16 + (b + 1) * 8)
            from_side = slice(side * half, (side + 1) * half)
            own_sum_ref[:, at, cols] = own_sum[from_side].reshape(groups, 8, HEAD)
            other_sum_ref[:, at, cols] = other_sum[from_side].reshape(groups, 8, HEAD)

    jobs = [(b, h) for b in range(samples) for h in range(heads)]
    ahead = products(*jobs[0])
    behind = None
    for at, job in enumerate(jobs):
        now = ahead
        if at + 1 < len(jobs):
            ahead = products(*jobs[at + 1])
        if behind is not None:
            add_up(*behind)
        behind = weigh(*job, *now)
    add_up(*behind)


def attend_kernel(core_ref, own_ref, other_ref, probs_ref, dscore_ref, attended_ref, query_grad_ref, held_ref, sent):
    samples, heads = probs_ref.shape[:2]
    first_core = core_ref[0] == 0
    features = heads * HEAD
    copies = []
    for b in range(samples):
        for h in range(heads):
            cols = slice(h * HEAD, (h + 1) * HEAD)
            value = text_of(own_ref, other_ref, first_core, b, features + h * HEAD)
            held_ref[0, b, :, cols] = dot(probs_ref[b, h], value, 0, 0).astype(BF16)
            key = text_of(own_ref, other_ref, first_core, b, h * HEAD)
            held_ref[1, b, :, cols] = dot(dscore_ref[b, h], key, 0, 0).astype(BF16)
        for which, ref in enumerate((attended_ref, query_grad_ref)):
            copy = pltpu.make_async_copy(held_ref.at[which, b], ref.at[b], sent.at[which, b])
            copy.start()
            copies.append(copy)
    for copy in copies:
        copy.wait()


def pair_sum_kernel(own_ref, other_ref, out_ref):
    out_ref[...] = (own_ref[...] + other_ref[...].astype(F32)).astype(BF16)


def total_kernel(parts_ref, out_ref):
    total = parts_ref[0].astype(F32)
    for g in range(1, parts_ref.shape[0]):
        total = total + parts_ref[g].astype(F32)
    total = total.astype(BF16)
    for g in range(out_ref.shape[0]):
        out_ref[g] = total


def weight_kernel(core_ref, columns_ref, total_ref, own_raw_ref, other_raw_ref, square_ref):
    groups, rows, features = total_ref.shape
    half = rows // 2
    core = core_ref[0]
    squares = None
    for raw_ref, feature_core in ((own_raw_ref, core), (other_raw_ref, 1 - core)):
        first = pl.multiple_of(feature_core * HEAD, HEAD)
        raw = None
        for which, side in ((0, core), (1, 1 - core)):
            text = columns_ref[which, :, :, pl.ds(first, HEAD)].reshape(groups * half, HEAD)
            total = total_ref[:, pl.ds(pl.multiple_of(side * half, half), half), :].reshape(groups * half, features)
            part = dot(text, total, 0, 0)
            raw = part if raw is None else raw + part
        raw_ref[...] = raw
        part = jnp.sum((raw * raw).reshape(-1, 8, features), axis=0)
        squares = part if squares is None else squares + part
    lanes = squares[:, :HEAD]
    for at in range(HEAD, features, HEAD):
        lanes = lanes + squares[:, at : at + HEAD]
    square_ref[...] = jnp.broadcast_to(jnp.sum(lanes, keepdims=True), square_ref.shape)


def scale_kernel(core_ref, own_ref, other_ref, squares_ref, key_ref, value_ref):
    overall = jnp.sum(squares_ref[...], keepdims=True)
    spread = jnp.sqrt(overall / (2.0 * DT * HEADS * HEAD) + 1e-06)
    factor = 1.0 / jnp.maximum(spread, 1.0)
    first_core = core_ref[0] == 0
    own = own_ref[...]
    other = other_ref[...]
    key_ref[...] = jnp.where(first_core, own, other) * factor
    value_ref[...] = jnp.where(first_core, other, own) * factor


def call(kernel, out, *args, scalars=0, far=0, far_out=False, scratch=(), mib=12):
    near, away = [pl.BlockSpec(memory_space=space) for space in (pltpu.VMEM, pl.ANY)]
    specs = [pl.BlockSpec(memory_space=pltpu.SMEM)] * scalars + [near] * (len(args) - scalars - far) + [away] * far
    out_spec = away if far_out else near
    return pl.pallas_call(
        kernel, out_shape=out, in_specs=specs, out_specs=out_spec if isinstance(out, jax.ShapeDtypeStruct) else [out_spec] * len(out),
        scratch_shapes=scratch, compiler_params=pltpu.CompilerParams(vmem_limit_bytes=int(mib * 1048576)),
    )(*args)


def shape(dims, dtype):
    return jax.ShapeDtypeStruct(dims, dtype)


def swap(array):
    return lax.ppermute(array, "core", [(0, 1), (1, 0)])


def exchange(array, axes):
    return lax.all_to_all(array, axes, 0, 0, tiled=True)


def per_device(video_query, text_states, key_weight, value_weight, text_lengths, output_grad):
    samples, video_rows, features = video_query.shape
    text_rows = samples * text_states.shape[1]
    groups = lax.axis_size(ZY)
    wide = 2 * features
    core = lax.axis_index("core").astype(jnp.int32).reshape(1)
    packed = call(
        project_kernel, shape((groups, text_rows, wide + DT // groups), BF16), text_states, key_weight, value_weight, far=3, mib=61,
        scratch=[
            pltpu.VMEM(text_states.shape, BF16), pltpu.VMEM((DT, wide), BF16),
            pltpu.SemaphoreType.DMA((2, CHUNKS)), pltpu.SemaphoreType.DMA,
        ],
    )
    own = exchange(packed, ZY)
    other = swap(own)
    like = shape(video_query.shape, BF16)
    block = (groups, 2 * text_rows, features)
    tall = shape((samples, features // HEAD, 2 * groups * 8, video_rows), BF16)
    own_sum, other_sum, probs, dscore, columns = call(
        score_kernel, [shape(block, F32), shape(block, BF16), tall, tall, shape((2, groups, text_rows, DT // groups), BF16)],
        text_lengths, core, video_query, output_grad, own, other, scalars=2,
    )
    attended, query_grad = call(
        attend_kernel, [like, like], core, own, other, probs, dscore, scalars=1, far_out=True,
        scratch=[pltpu.VMEM((2,) + video_query.shape, BF16), pltpu.SemaphoreType.DMA((2, samples))],
    )
    pair = call(pair_sum_kernel, shape(block, BF16), own_sum, swap(other_sum))
    parts = exchange(pair, ZY)
    totals = exchange(call(total_kernel, shape(block, BF16), parts), ZY)
    every = lax.axis_size(ALL)
    weight = shape((HEAD, features), F32)
    own_raw, other_raw, squares = call(
        weight_kernel, [weight, weight, shape((every, 1), F32)], core, columns, totals, scalars=1,
    )
    squares = exchange(squares, ALL)
    key_weight_grad, value_weight_grad = call(
        scale_kernel, [weight, weight], core, own_raw, swap(other_raw), squares, scalars=1,
    )
    return attended, query_grad, key_weight_grad, value_weight_grad


def solution(mesh):
    split = Mesh(mesh.devices.reshape(8, 2, 2, 2, 4), ALL)
    return jax.shard_map(
        per_device,
        mesh=split,
        in_specs=(P(None, SEQ, TP), P(None, SEQ, None), P(None, TP), P(None, TP), P(), P(None, SEQ, TP)),
        out_specs=(P(None, SEQ, TP), P(None, SEQ, TP), P(SEQ, TP), P(SEQ, TP)),
        check_vma=False,
    )
```

```python
import math

import jax
import jax.numpy as jnp
from jax import lax
from jax.experimental import pallas as pl
from jax.experimental.pallas import tpu as pltpu
from jax.sharding import Mesh
from jax.sharding import PartitionSpec as P


DT = 4096
HEADS = 24
HEAD = 128
CHUNKS = 2
YZ = ("yh", "z")
SEQ = ("z", "yh", "core")
TP = ("yl", "x")
ALL = SEQ + TP
SCALING = 1.0 / math.sqrt(HEAD)
BF16 = jnp.bfloat16
F32 = jnp.float32


def position(group, groups):
    return group % (groups // 2) * 2 + group // (groups // 2)


def dot(a, b, ca, cb):
    return lax.dot_general(a, b, (((ca,), (cb,)), ((), ())), preferred_element_type=F32)


def project_kernel(text_ref, key_ref, value_ref, out_ref, states_ref, held_ref, arrived, here):
    groups = out_ref.shape[0]
    features = key_ref.shape[1]
    step = DT // CHUNKS
    states = pltpu.make_async_copy(text_ref, states_ref, here)
    states.start()
    copies = []
    for at in range(CHUNKS):
        rows = pl.ds(at * step, step)
        for which, ref in enumerate((key_ref, value_ref)):
            copy = pltpu.make_async_copy(ref.at[rows], held_ref.at[rows, pl.ds(which * features, features)], arrived.at[which, at])
            copy.start()
            copies.append(copy)
    states.wait()
    text = states_ref[...].reshape(-1, DT)
    wide = DT // groups
    for g in range(groups):
        first = position(g, groups) * wide
        out_ref[g, :, 2 * features :] = text[:, first : first + wide]
    total = None
    for at in range(CHUNKS):
        rows = slice(at * step, (at + 1) * step)
        copies[2 * at].wait()
        copies[2 * at + 1].wait()
        part = dot(text[:, rows], held_ref[rows], 1, 0)
        total = part if total is None else total + part
    total = total.astype(BF16)
    for g in range(groups):
        out_ref[g, :, : 2 * features] = total


def text_of(own_ref, other_ref, first_core, b, first):
    half = own_ref.shape[0] * 8
    own, other = [ref[:, b * 8 : (b + 1) * 8, first : first + HEAD].reshape(half, HEAD) for ref in (own_ref, other_ref)]
    return jnp.concatenate([jnp.where(first_core, own, other), jnp.where(first_core, other, own)], axis=0)


def score_kernel(lengths_ref, core_ref, query_ref, grad_ref, own_ref, other_ref, own_sum_ref, other_sum_ref, probs_ref, dscore_ref, columns_ref):
    samples, _, features = query_ref.shape
    groups = own_ref.shape[0]
    heads = features // HEAD
    first_core = core_ref[0] == 0
    half = groups * 8
    place = lax.broadcasted_iota(jnp.int32, (2 * half, 1), 0)
    within = place % half
    token = position(within // 8, groups) * 16 + (place // half) * 8 + within % 8
    columns_ref[0] = own_ref[:, :, 2 * features :]
    columns_ref[1] = other_ref[:, :, 2 * features :]

    def products(b, h):
        cols = slice(h * HEAD, (h + 1) * HEAD)
        key = text_of(own_ref, other_ref, first_core, b, h * HEAD)
        value = text_of(own_ref, other_ref, first_core, b, features + h * HEAD)
        return dot(key, query_ref[b, :, cols], 1, 1), dot(value, grad_ref[b, :, cols], 1, 1)

    def weigh(b, h, scores, dprob):
        scores = jnp.where(token < lengths_ref[b], scores * SCALING, -1e30)
        weights = jnp.exp(scores - jnp.max(scores, axis=0, keepdims=True))
        probs = weights * (1.0 / jnp.sum(weights, axis=0, keepdims=True))
        probs_low = probs.astype(BF16)
        delta = jnp.sum(probs * dprob, axis=0, keepdims=True)
        dscore = (probs * (dprob - delta) * SCALING).astype(BF16)
        probs_ref[b, h] = probs_low
        dscore_ref[b, h] = dscore
        return b, h, probs_low, dscore

    def add_up(b, h, probs_low, dscore):
        cols = slice(h * HEAD, (h + 1) * HEAD)
        key_sum = dot(dscore, query_ref[b, :, cols], 1, 0)
        value_sum = dot(probs_low, grad_ref[b, :, cols], 1, 0)
        own_sum = jnp.where(first_core, key_sum, value_sum)
        other_sum = jnp.where(first_core, value_sum, key_sum).astype(BF16)
        for side in range(2):
            at = slice(side * 16 + b * 8, side * 16 + (b + 1) * 8)
            from_side = slice(side * half, (side + 1) * half)
            own_sum_ref[:, at, cols] = own_sum[from_side].reshape(groups, 8, HEAD)
            other_sum_ref[:, at, cols] = other_sum[from_side].reshape(groups, 8, HEAD)

    jobs = [(b, h) for b in range(samples) for h in range(heads)]
    ahead = products(*jobs[0])
    behind = None
    for at, job in enumerate(jobs):
        now = ahead
        if at + 1 < len(jobs):
            ahead = products(*jobs[at + 1])
        if behind is not None:
            add_up(*behind)
        behind = weigh(*job, *now)
    add_up(*behind)


def attend_kernel(core_ref, own_ref, other_ref, probs_ref, dscore_ref, attended_ref, query_grad_ref, held_ref, sent):
    samples, heads = probs_ref.shape[:2]
    first_core = core_ref[0] == 0
    features = heads * HEAD
    copies = []
    for b in range(samples):
        for h in range(heads):
            cols = slice(h * HEAD, (h + 1) * HEAD)
            value = text_of(own_ref, other_ref, first_core, b, features + h * HEAD)
            held_ref[0, b, :, cols] = dot(probs_ref[b, h], value, 0, 0).astype(BF16)
            key = text_of(own_ref, other_ref, first_core, b, h * HEAD)
            held_ref[1, b, :, cols] = dot(dscore_ref[b, h], key, 0, 0).astype(BF16)
        for which, ref in enumerate((attended_ref, query_grad_ref)):
            copy = pltpu.make_async_copy(held_ref.at[which, b], ref.at[b], sent.at[which, b])
            copy.start()
            copies.append(copy)
    for copy in copies:
        copy.wait()


def pair_sum_kernel(own_ref, other_ref, out_ref):
    out_ref[...] = (own_ref[...] + other_ref[...].astype(F32)).astype(BF16)


def total_kernel(parts_ref, out_ref):
    total = parts_ref[0].astype(F32)
    for g in range(1, parts_ref.shape[0]):
        total = total + parts_ref[g].astype(F32)
    total = total.astype(BF16)
    for g in range(out_ref.shape[0]):
        out_ref[g] = total


def weight_kernel(core_ref, columns_ref, total_ref, own_raw_ref, other_raw_ref, square_ref):
    groups, rows, features = total_ref.shape
    half = rows // 2
    core = core_ref[0]
    squares = None
    for raw_ref, feature_core in ((own_raw_ref, core), (other_raw_ref, 1 - core)):
        first = pl.multiple_of(feature_core * HEAD, HEAD)
        raw = None
        for which, side in ((0, core), (1, 1 - core)):
            text = columns_ref[which, :, :, pl.ds(first, HEAD)].reshape(groups * half, HEAD)
            total = total_ref[:, pl.ds(pl.multiple_of(side * half, half), half), :].reshape(groups * half, features)
            part = dot(text, total, 0, 0)
            raw = part if raw is None else raw + part
        raw_ref[...] = raw
        part = jnp.sum((raw * raw).reshape(-1, 8, features), axis=0)
        squares = part if squares is None else squares + part
    lanes = squares[:, :HEAD]
    for at in range(HEAD, features, HEAD):
        lanes = lanes + squares[:, at : at + HEAD]
    square_ref[...] = jnp.broadcast_to(jnp.sum(lanes, keepdims=True), square_ref.shape)


def scale_kernel(core_ref, own_ref, other_ref, squares_ref, key_ref, value_ref):
    overall = jnp.sum(squares_ref[...], keepdims=True)
    spread = jnp.sqrt(overall / (2.0 * DT * HEADS * HEAD) + 1e-06)
    factor = 1.0 / jnp.maximum(spread, 1.0)
    first_core = core_ref[0] == 0
    own = own_ref[...]
    other = other_ref[...]
    key_ref[...] = jnp.where(first_core, own, other) * factor
    value_ref[...] = jnp.where(first_core, other, own) * factor


def call(kernel, out, *args, scalars=0, far=0, far_out=False, scratch=(), mib=12):
    near, away = [pl.BlockSpec(memory_space=space) for space in (pltpu.VMEM, pl.ANY)]
    specs = [pl.BlockSpec(memory_space=pltpu.SMEM)] * scalars + [near] * (len(args) - scalars - far) + [away] * far
    out_spec = away if far_out else near
    return pl.pallas_call(
        kernel, out_shape=out, in_specs=specs, out_specs=out_spec if isinstance(out, jax.ShapeDtypeStruct) else [out_spec] * len(out),
        scratch_shapes=scratch, compiler_params=pltpu.CompilerParams(vmem_limit_bytes=int(mib * 1048576)),
    )(*args)


def shape(dims, dtype):
    return jax.ShapeDtypeStruct(dims, dtype)


def swap(array):
    return lax.ppermute(array, "core", [(0, 1), (1, 0)])


def exchange(array, axes):
    return lax.all_to_all(array, axes, 0, 0, tiled=True)


def per_device(video_query, text_states, key_weight, value_weight, text_lengths, output_grad):
    samples, video_rows, features = video_query.shape
    text_rows = samples * text_states.shape[1]
    groups = lax.axis_size(YZ)
    wide = 2 * features
    core = lax.axis_index("core").astype(jnp.int32).reshape(1)
    packed = call(
        project_kernel, shape((groups, text_rows, wide + DT // groups), BF16), text_states, key_weight, value_weight, far=3, mib=61,
        scratch=[
            pltpu.VMEM(text_states.shape, BF16), pltpu.VMEM((DT, wide), BF16),
            pltpu.SemaphoreType.DMA((2, CHUNKS)), pltpu.SemaphoreType.DMA,
        ],
    )
    own = exchange(packed, YZ)
    other = swap(own)
    like = shape(video_query.shape, BF16)
    block = (groups, 2 * text_rows, features)
    tall = shape((samples, features // HEAD, 2 * groups * 8, video_rows), BF16)
    own_sum, other_sum, probs, dscore, columns = call(
        score_kernel, [shape(block, F32), shape(block, BF16), tall, tall, shape((2, groups, text_rows, DT // groups), BF16)],
        text_lengths, core, video_query, output_grad, own, other, scalars=2,
    )
    attended, query_grad = call(
        attend_kernel, [like, like], core, own, other, probs, dscore, scalars=1, far_out=True,
        scratch=[pltpu.VMEM((2,) + video_query.shape, BF16), pltpu.SemaphoreType.DMA((2, samples))],
    )
    pair = call(pair_sum_kernel, shape(block, BF16), own_sum, swap(other_sum))
    parts = exchange(pair, YZ)
    totals = exchange(call(total_kernel, shape(block, BF16), parts), YZ)
    every = lax.axis_size(ALL)
    weight = shape((HEAD, features), F32)
    own_raw, other_raw, squares = call(
        weight_kernel, [weight, weight, shape((every, 1), F32)], core, columns, totals, scalars=1,
    )
    squares = exchange(squares, ALL)
    key_weight_grad, value_weight_grad = call(
        scale_kernel, [weight, weight], core, own_raw, swap(other_raw), squares, scalars=1,
    )
    return attended, query_grad, key_weight_grad, value_weight_grad


def solution(mesh):
    split = Mesh(mesh.devices.reshape(8, 2, 2, 2, 4), ALL)
    return jax.shard_map(
        per_device,
        mesh=split,
        in_specs=(P(None, SEQ, TP), P(None, SEQ, None), P(None, TP), P(None, TP), P(), P(None, SEQ, TP)),
        out_specs=(P(None, SEQ, TP), P(None, SEQ, TP), P(SEQ, TP), P(SEQ, TP)),
        check_vma=False,
    )
```

```python
import math

import jax
import jax.numpy as jnp
from jax import lax
from jax.experimental import pallas as pl
from jax.experimental.pallas import tpu as pltpu
from jax.sharding import Mesh
from jax.sharding import PartitionSpec as P


DT = 4096
HEADS = 24
HEAD = 128
CHUNKS = 2
YZ = ("yh", "z")
SEQ = ("z", "yh", "core")
TP = ("yl", "x")
ALL = SEQ + TP
SCALING = 1.0 / math.sqrt(HEAD)
BF16 = jnp.bfloat16
F32 = jnp.float32


def position(group, groups):
    return group % (groups // 2) * 2 + group // (groups // 2)


def dot(a, b, ca, cb):
    return lax.dot_general(a, b, (((ca,), (cb,)), ((), ())), preferred_element_type=F32)


def project_kernel(text_ref, key_ref, value_ref, out_ref, states_ref, held_ref, arrived, here):
    groups = out_ref.shape[0]
    features = key_ref.shape[1]
    step = DT // CHUNKS
    states = pltpu.make_async_copy(text_ref, states_ref, here)
    states.start()
    copies = []
    for at in range(CHUNKS):
        rows = pl.ds(at * step, step)
        for which, ref in enumerate((key_ref, value_ref)):
            copy = pltpu.make_async_copy(ref.at[rows], held_ref.at[rows, pl.ds(which * features, features)], arrived.at[which, at])
            copy.start()
            copies.append(copy)
    states.wait()
    text = states_ref[...].reshape(-1, DT)
    wide = DT // groups
    for g in range(groups):
        first = position(g, groups) * wide
        out_ref[g, :, 2 * features :] = text[:, first : first + wide]
    total = None
    for at in range(CHUNKS):
        rows = slice(at * step, (at + 1) * step)
        copies[2 * at].wait()
        copies[2 * at + 1].wait()
        part = dot(text[:, rows], held_ref[rows], 1, 0)
        total = part if total is None else total + part
    total = total.astype(BF16)
    for g in range(groups):
        out_ref[g, :, : 2 * features] = total


def text_of(own_ref, other_ref, first_core, b, first):
    half = own_ref.shape[0] * 8
    own, other = [ref[:, b * 8 : (b + 1) * 8, first : first + HEAD].reshape(half, HEAD) for ref in (own_ref, other_ref)]
    return jnp.concatenate([jnp.where(first_core, own, other), jnp.where(first_core, other, own)], axis=0)


def score_kernel(lengths_ref, core_ref, query_ref, grad_ref, own_ref, other_ref, own_sum_ref, other_sum_ref, probs_ref, dscore_ref, columns_ref):
    samples, _, features = query_ref.shape
    groups = own_ref.shape[0]
    heads = features // HEAD
    first_core = core_ref[0] == 0
    half = groups * 8
    place = lax.broadcasted_iota(jnp.int32, (2 * half, 1), 0)
    within = place % half
    token = position(within // 8, groups) * 16 + (place // half) * 8 + within % 8
    columns_ref[0] = own_ref[:, :, 2 * features :]
    columns_ref[1] = other_ref[:, :, 2 * features :]

    def products(b, h):
        cols = slice(h * HEAD, (h + 1) * HEAD)
        key = text_of(own_ref, other_ref, first_core, b, h * HEAD)
        value = text_of(own_ref, other_ref, first_core, b, features + h * HEAD)
        return dot(key, query_ref[b, :, cols], 1, 1), dot(value, grad_ref[b, :, cols], 1, 1)

    def weigh(b, h, scores, dprob):
        scores = jnp.where(token < lengths_ref[b], scores * SCALING, -1e30)
        weights = jnp.exp(scores - jnp.max(scores, axis=0, keepdims=True))
        probs = weights * (1.0 / jnp.sum(weights, axis=0, keepdims=True))
        probs_low = probs.astype(BF16)
        delta = jnp.sum(probs * dprob, axis=0, keepdims=True)
        dscore = (probs * (dprob - delta) * SCALING).astype(BF16)
        probs_ref[b, h] = probs_low
        dscore_ref[b, h] = dscore
        return b, h, probs_low, dscore

    def add_up(b, h, probs_low, dscore):
        cols = slice(h * HEAD, (h + 1) * HEAD)
        key_sum = dot(dscore, query_ref[b, :, cols], 1, 0)
        value_sum = dot(probs_low, grad_ref[b, :, cols], 1, 0)
        own_sum = jnp.where(first_core, key_sum, value_sum)
        other_sum = jnp.where(first_core, value_sum, key_sum).astype(BF16)
        for side in range(2):
            at = slice(side * 16 + b * 8, side * 16 + (b + 1) * 8)
            from_side = slice(side * half, (side + 1) * half)
            own_sum_ref[:, at, cols] = own_sum[from_side].reshape(groups, 8, HEAD)
            other_sum_ref[:, at, cols] = other_sum[from_side].reshape(groups, 8, HEAD)

    jobs = [(b, h) for b in range(samples) for h in range(heads)]
    ahead = products(*jobs[0])
    behind = None
    for at, job in enumerate(jobs):
        now = ahead
        if at + 1 < len(jobs):
            ahead = products(*jobs[at + 1])
        if behind is not None:
            add_up(*behind)
        behind = weigh(*job, *now)
    add_up(*behind)


def attend_kernel(core_ref, own_ref, other_ref, probs_ref, dscore_ref, attended_ref, query_grad_ref, held_ref, sent):
    samples, heads = probs_ref.shape[:2]
    first_core = core_ref[0] == 0
    features = heads * HEAD
    copies = []
    for b in range(samples):
        for h in range(heads):
            cols = slice(h * HEAD, (h + 1) * HEAD)
            value = text_of(own_ref, other_ref, first_core, b, features + h * HEAD)
            held_ref[0, b, :, cols] = dot(probs_ref[b, h], value, 0, 0).astype(BF16)
            key = text_of(own_ref, other_ref, first_core, b, h * HEAD)
            held_ref[1, b, :, cols] = dot(dscore_ref[b, h], key, 0, 0).astype(BF16)
            part = pl.ds(h * HEAD, HEAD)
            for which, ref in enumerate((attended_ref, query_grad_ref)):
                copy = pltpu.make_async_copy(held_ref.at[which, b, :, part], ref.at[b, :, part], sent.at[which, b * heads + h])
                copy.start()
                copies.append(copy)
    for copy in copies:
        copy.wait()


def pair_sum_kernel(own_ref, other_ref, out_ref):
    out_ref[...] = (own_ref[...] + other_ref[...].astype(F32)).astype(BF16)


def total_kernel(parts_ref, out_ref):
    total = parts_ref[0].astype(F32)
    for g in range(1, parts_ref.shape[0]):
        total = total + parts_ref[g].astype(F32)
    total = total.astype(BF16)
    for g in range(out_ref.shape[0]):
        out_ref[g] = total


def weight_kernel(core_ref, columns_ref, total_ref, own_raw_ref, other_raw_ref, square_ref):
    groups, rows, features = total_ref.shape
    half = rows // 2
    core = core_ref[0]
    squares = None
    for raw_ref, feature_core in ((own_raw_ref, core), (other_raw_ref, 1 - core)):
        first = pl.multiple_of(feature_core * HEAD, HEAD)
        raw = None
        for which, side in ((0, core), (1, 1 - core)):
            text = columns_ref[which, :, :, pl.ds(first, HEAD)].reshape(groups * half, HEAD)
            total = total_ref[:, pl.ds(pl.multiple_of(side * half, half), half), :].reshape(groups * half, features)
            part = dot(text, total, 0, 0)
            raw = part if raw is None else raw + part
        raw_ref[...] = raw
        part = jnp.sum((raw * raw).reshape(-1, 8, features), axis=0)
        squares = part if squares is None else squares + part
    lanes = squares[:, :HEAD]
    for at in range(HEAD, features, HEAD):
        lanes = lanes + squares[:, at : at + HEAD]
    square_ref[...] = jnp.broadcast_to(jnp.sum(lanes, keepdims=True), square_ref.shape)


def scale_kernel(core_ref, own_ref, other_ref, squares_ref, key_ref, value_ref):
    overall = jnp.sum(squares_ref[...], keepdims=True)
    spread = jnp.sqrt(overall / (2.0 * DT * HEADS * HEAD) + 1e-06)
    factor = 1.0 / jnp.maximum(spread, 1.0)
    first_core = core_ref[0] == 0
    own = own_ref[...]
    other = other_ref[...]
    key_ref[...] = jnp.where(first_core, own, other) * factor
    value_ref[...] = jnp.where(first_core, other, own) * factor


def call(kernel, out, *args, scalars=0, far=0, far_out=False, scratch=(), mib=12):
    near, away = [pl.BlockSpec(memory_space=space) for space in (pltpu.VMEM, pl.ANY)]
    specs = [pl.BlockSpec(memory_space=pltpu.SMEM)] * scalars + [near] * (len(args) - scalars - far) + [away] * far
    out_spec = away if far_out else near
    return pl.pallas_call(
        kernel, out_shape=out, in_specs=specs, out_specs=out_spec if isinstance(out, jax.ShapeDtypeStruct) else [out_spec] * len(out),
        scratch_shapes=scratch, compiler_params=pltpu.CompilerParams(vmem_limit_bytes=int(mib * 1048576)),
    )(*args)


def shape(dims, dtype):
    return jax.ShapeDtypeStruct(dims, dtype)


def swap(array):
    return lax.ppermute(array, "core", [(0, 1), (1, 0)])


def exchange(array, axes):
    return lax.all_to_all(array, axes, 0, 0, tiled=True)


def per_device(video_query, text_states, key_weight, value_weight, text_lengths, output_grad):
    samples, video_rows, features = video_query.shape
    text_rows = samples * text_states.shape[1]
    groups = lax.axis_size(YZ)
    wide = 2 * features
    core = lax.axis_index("core").astype(jnp.int32).reshape(1)
    packed = call(
        project_kernel, shape((groups, text_rows, wide + DT // groups), BF16), text_states, key_weight, value_weight, far=3, mib=61,
        scratch=[
            pltpu.VMEM(text_states.shape, BF16), pltpu.VMEM((DT, wide), BF16),
            pltpu.SemaphoreType.DMA((2, CHUNKS)), pltpu.SemaphoreType.DMA,
        ],
    )
    own = exchange(packed, YZ)
    other = swap(own)
    like = shape(video_query.shape, BF16)
    block = (groups, 2 * text_rows, features)
    tall = shape((samples, features // HEAD, 2 * groups * 8, video_rows), BF16)
    own_sum, other_sum, probs, dscore, columns = call(
        score_kernel, [shape(block, F32), shape(block, BF16), tall, tall, shape((2, groups, text_rows, DT // groups), BF16)],
        text_lengths, core, video_query, output_grad, own, other, scalars=2,
    )
    attended, query_grad = call(
        attend_kernel, [like, like], core, own, other, probs, dscore, scalars=1, far_out=True,
        scratch=[pltpu.VMEM((2,) + video_query.shape, BF16), pltpu.SemaphoreType.DMA((2, samples * features // HEAD))],
    )
    pair = call(pair_sum_kernel, shape(block, BF16), own_sum, swap(other_sum))
    parts = exchange(pair, YZ)
    totals = exchange(call(total_kernel, shape(block, BF16), parts), YZ)
    every = lax.axis_size(ALL)
    weight = shape((HEAD, features), F32)
    own_raw, other_raw, squares = call(
        weight_kernel, [weight, weight, shape((every, 1), F32)], core, columns, totals, scalars=1,
    )
    squares = exchange(squares, ALL)
    key_weight_grad, value_weight_grad = call(
        scale_kernel, [weight, weight], core, own_raw, swap(other_raw), squares, scalars=1,
    )
    return attended, query_grad, key_weight_grad, value_weight_grad


def solution(mesh):
    split = Mesh(mesh.devices.reshape(8, 2, 2, 2, 4), ALL)
    return jax.shard_map(
        per_device,
        mesh=split,
        in_specs=(P(None, SEQ, TP), P(None, SEQ, None), P(None, TP), P(None, TP), P(), P(None, SEQ, TP)),
        out_specs=(P(None, SEQ, TP), P(None, SEQ, TP), P(SEQ, TP), P(SEQ, TP)),
        check_vma=False,
    )
```

```python
import math

import jax
import jax.numpy as jnp
from jax import lax
from jax.experimental import pallas as pl
from jax.experimental.pallas import tpu as pltpu
from jax.sharding import Mesh
from jax.sharding import PartitionSpec as P


DT = 4096
HEADS = 24
HEAD = 128
CHUNKS = 2
YZ = ("yh", "z")
SEQ = ("z", "yh", "core")
TP = ("yl", "x")
ALL = SEQ + TP
SCALING = 1.0 / math.sqrt(HEAD)
BF16 = jnp.bfloat16
F32 = jnp.float32


def position(group, groups):
    return group % (groups // 2) * 2 + group // (groups // 2)


def dot(a, b, ca, cb):
    return lax.dot_general(a, b, (((ca,), (cb,)), ((), ())), preferred_element_type=F32)


def project_kernel(text_ref, key_ref, value_ref, out_ref, states_ref, held_ref, arrived, here):
    features = key_ref.shape[1]
    step = DT // CHUNKS
    states = pltpu.make_async_copy(text_ref, states_ref, here)
    states.start()
    copies = []
    for at in range(CHUNKS):
        rows = pl.ds(at * step, step)
        for which, ref in enumerate((key_ref, value_ref)):
            copy = pltpu.make_async_copy(ref.at[rows], held_ref.at[rows, pl.ds(which * features, features)], arrived.at[which, at])
            copy.start()
            copies.append(copy)
    states.wait()
    text = states_ref[...].reshape(-1, DT)
    total = None
    for at in range(CHUNKS):
        rows = slice(at * step, (at + 1) * step)
        copies[2 * at].wait()
        copies[2 * at + 1].wait()
        part = dot(text[:, rows], held_ref[rows], 1, 0)
        total = part if total is None else total + part
    out_ref[...] = total.astype(BF16)


def pack_kernel(text_ref, part_ref, out_ref):
    groups = out_ref.shape[0]
    features = part_ref.shape[1]
    wide = DT // groups
    text = text_ref[...].reshape(-1, DT)
    part = part_ref[...]
    for g in range(groups):
        first = position(g, groups) * wide
        out_ref[g, :, :features] = part
        out_ref[g, :, features:] = text[:, first : first + wide]


def text_of(own_ref, other_ref, first_core, b, first):
    half = own_ref.shape[0] * 8
    own, other = [ref[:, b * 8 : (b + 1) * 8, first : first + HEAD].reshape(half, HEAD) for ref in (own_ref, other_ref)]
    return jnp.concatenate([jnp.where(first_core, own, other), jnp.where(first_core, other, own)], axis=0)


def score_kernel(lengths_ref, core_ref, query_ref, grad_ref, own_ref, other_ref, own_sum_ref, other_sum_ref, probs_ref, dscore_ref, columns_ref):
    samples, _, features = query_ref.shape
    groups = own_ref.shape[0]
    heads = features // HEAD
    first_core = core_ref[0] == 0
    half = groups * 8
    place = lax.broadcasted_iota(jnp.int32, (2 * half, 1), 0)
    within = place % half
    token = position(within // 8, groups) * 16 + (place // half) * 8 + within % 8
    columns_ref[0] = own_ref[:, :, 2 * features :]
    columns_ref[1] = other_ref[:, :, 2 * features :]

    def products(b, h):
        cols = slice(h * HEAD, (h + 1) * HEAD)
        key = text_of(own_ref, other_ref, first_core, b, h * HEAD)
        value = text_of(own_ref, other_ref, first_core, b, features + h * HEAD)
        return dot(key, query_ref[b, :, cols], 1, 1), dot(value, grad_ref[b, :, cols], 1, 1)

    def weigh(b, h, scores, dprob):
        scores = jnp.where(token < lengths_ref[b], scores * SCALING, -1e30)
        weights = jnp.exp(scores - jnp.max(scores, axis=0, keepdims=True))
        probs = weights * (1.0 / jnp.sum(weights, axis=0, keepdims=True))
        probs_low = probs.astype(BF16)
        delta = jnp.sum(probs * dprob, axis=0, keepdims=True)
        dscore = (probs * (dprob - delta) * SCALING).astype(BF16)
        probs_ref[b, h] = probs_low
        dscore_ref[b, h] = dscore
        return b, h, probs_low, dscore

    def add_up(b, h, probs_low, dscore):
        cols = slice(h * HEAD, (h + 1) * HEAD)
        key_sum = dot(dscore, query_ref[b, :, cols], 1, 0)
        value_sum = dot(probs_low, grad_ref[b, :, cols], 1, 0)
        own_sum = jnp.where(first_core, key_sum, value_sum)
        other_sum = jnp.where(first_core, value_sum, key_sum).astype(BF16)
        for side in range(2):
            at = slice(side * 16 + b * 8, side * 16 + (b + 1) * 8)
            from_side = slice(side * half, (side + 1) * half)
            own_sum_ref[:, at, cols] = own_sum[from_side].reshape(groups, 8, HEAD)
            other_sum_ref[:, at, cols] = other_sum[from_side].reshape(groups, 8, HEAD)

    jobs = [(b, h) for b in range(samples) for h in range(heads)]
    ahead = products(*jobs[0])
    behind = None
    for at, job in enumerate(jobs):
        now = ahead
        if at + 1 < len(jobs):
            ahead = products(*jobs[at + 1])
        if behind is not None:
            add_up(*behind)
        behind = weigh(*job, *now)
    add_up(*behind)


def attend_kernel(core_ref, own_ref, other_ref, probs_ref, dscore_ref, attended_ref, query_grad_ref, held_ref, sent):
    samples, heads = probs_ref.shape[:2]
    first_core = core_ref[0] == 0
    features = heads * HEAD
    copies = []
    for b in range(samples):
        for h in range(heads):
            cols = slice(h * HEAD, (h + 1) * HEAD)
            value = text_of(own_ref, other_ref, first_core, b, features + h * HEAD)
            held_ref[0, b, :, cols] = dot(probs_ref[b, h], value, 0, 0).astype(BF16)
            key = text_of(own_ref, other_ref, first_core, b, h * HEAD)
            held_ref[1, b, :, cols] = dot(dscore_ref[b, h], key, 0, 0).astype(BF16)
            part = pl.ds(h * HEAD, HEAD)
            for which, ref in enumerate((attended_ref, query_grad_ref)):
                copy = pltpu.make_async_copy(held_ref.at[which, b, :, part], ref.at[b, :, part], sent.at[which, b * heads + h])
                copy.start()
                copies.append(copy)
    for copy in copies:
        copy.wait()


def pair_sum_kernel(own_ref, other_ref, out_ref):
    out_ref[...] = (own_ref[...] + other_ref[...].astype(F32)).astype(BF16)


def total_kernel(parts_ref, out_ref):
    total = parts_ref[0].astype(F32)
    for g in range(1, parts_ref.shape[0]):
        total = total + parts_ref[g].astype(F32)
    total = total.astype(BF16)
    for g in range(out_ref.shape[0]):
        out_ref[g] = total


def weight_kernel(core_ref, columns_ref, total_ref, own_raw_ref, other_raw_ref, square_ref):
    groups, rows, features = total_ref.shape
    half = rows // 2
    core = core_ref[0]
    squares = None
    for raw_ref, feature_core in ((own_raw_ref, core), (other_raw_ref, 1 - core)):
        first = pl.multiple_of(feature_core * HEAD, HEAD)
        raw = None
        for which, side in ((0, core), (1, 1 - core)):
            text = columns_ref[which, :, :, pl.ds(first, HEAD)].reshape(groups * half, HEAD)
            total = total_ref[:, pl.ds(pl.multiple_of(side * half, half), half), :].reshape(groups * half, features)
            part = dot(text, total, 0, 0)
            raw = part if raw is None else raw + part
        raw_ref[...] = raw
        part = jnp.sum((raw * raw).reshape(-1, 8, features), axis=0)
        squares = part if squares is None else squares + part
    lanes = squares[:, :HEAD]
    for at in range(HEAD, features, HEAD):
        lanes = lanes + squares[:, at : at + HEAD]
    square_ref[...] = jnp.broadcast_to(jnp.sum(lanes, keepdims=True), square_ref.shape)


def scale_kernel(core_ref, own_ref, other_ref, squares_ref, key_ref, value_ref):
    overall = jnp.sum(squares_ref[...], keepdims=True)
    spread = jnp.sqrt(overall / (2.0 * DT * HEADS * HEAD) + 1e-06)
    factor = 1.0 / jnp.maximum(spread, 1.0)
    first_core = core_ref[0] == 0
    own = own_ref[...]
    other = other_ref[...]
    key_ref[...] = jnp.where(first_core, own, other) * factor
    value_ref[...] = jnp.where(first_core, other, own) * factor


def call(kernel, out, *args, scalars=0, far=0, far_out=False, scratch=(), mib=12):
    near, away = [pl.BlockSpec(memory_space=space) for space in (pltpu.VMEM, pl.ANY)]
    specs = [pl.BlockSpec(memory_space=pltpu.SMEM)] * scalars + [near] * (len(args) - scalars - far) + [away] * far
    out_spec = away if far_out else near
    return pl.pallas_call(
        kernel, out_shape=out, in_specs=specs, out_specs=out_spec if isinstance(out, jax.ShapeDtypeStruct) else [out_spec] * len(out),
        scratch_shapes=scratch, compiler_params=pltpu.CompilerParams(vmem_limit_bytes=int(mib * 1048576)),
    )(*args)


def shape(dims, dtype):
    return jax.ShapeDtypeStruct(dims, dtype)


def swap(array):
    return lax.ppermute(array, "core", [(0, 1), (1, 0)])


def exchange(array, axes):
    return lax.all_to_all(array, axes, 0, 0, tiled=True)


def per_device(video_query, text_states, key_weight, value_weight, text_lengths, output_grad):
    samples, video_rows, features = video_query.shape
    text_rows = samples * text_states.shape[1]
    groups = lax.axis_size(YZ)
    wide = 2 * features
    core = lax.axis_index("core").astype(jnp.int32).reshape(1)
    part = call(
        project_kernel, shape((text_rows, wide), BF16), text_states, key_weight, value_weight, far=3, mib=53.5,
        scratch=[
            pltpu.VMEM(text_states.shape, BF16), pltpu.VMEM((DT, wide), BF16),
            pltpu.SemaphoreType.DMA((2, CHUNKS)), pltpu.SemaphoreType.DMA,
        ],
    )
    packed = call(pack_kernel, shape((groups, text_rows, wide + DT // groups), BF16), text_states, part)
    own = exchange(packed, YZ)
    other = swap(own)
    like = shape(video_query.shape, BF16)
    block = (groups, 2 * text_rows, features)
    tall = shape((samples, features // HEAD, 2 * groups * 8, video_rows), BF16)
    own_sum, other_sum, probs, dscore, columns = call(
        score_kernel, [shape(block, F32), shape(block, BF16), tall, tall, shape((2, groups, text_rows, DT // groups), BF16)],
        text_lengths, core, video_query, output_grad, own, other, scalars=2,
    )
    attended, query_grad = call(
        attend_kernel, [like, like], core, own, other, probs, dscore, scalars=1, far_out=True,
        scratch=[pltpu.VMEM((2,) + video_query.shape, BF16), pltpu.SemaphoreType.DMA((2, samples * features // HEAD))],
    )
    pair = call(pair_sum_kernel, shape(block, BF16), own_sum, swap(other_sum))
    parts = exchange(pair, YZ)
    totals = exchange(call(total_kernel, shape(block, BF16), parts), YZ)
    every = lax.axis_size(ALL)
    weight = shape((HEAD, features), F32)
    own_raw, other_raw, squares = call(
        weight_kernel, [weight, weight, shape((every, 1), F32)], core, columns, totals, scalars=1,
    )
    squares = exchange(squares, ALL)
    key_weight_grad, value_weight_grad = call(
        scale_kernel, [weight, weight], core, own_raw, swap(other_raw), squares, scalars=1,
    )
    return attended, query_grad, key_weight_grad, value_weight_grad


def solution(mesh):
    split = Mesh(mesh.devices.reshape(8, 2, 2, 2, 4), ALL)
    return jax.shard_map(
        per_device,
        mesh=split,
        in_specs=(P(None, SEQ, TP), P(None, SEQ, None), P(None, TP), P(None, TP), P(), P(None, SEQ, TP)),
        out_specs=(P(None, SEQ, TP), P(None, SEQ, TP), P(SEQ, TP), P(SEQ, TP)),
        check_vma=False,
    )
```

```python
import math

import jax
import jax.numpy as jnp
from jax import lax
from jax.experimental import pallas as pl
from jax.experimental.pallas import tpu as pltpu
from jax.sharding import Mesh
from jax.sharding import PartitionSpec as P


DT = 4096
HEADS = 24
HEAD = 128
CHUNKS = 2
YZ = ("yh", "z")
SEQ = ("z", "yh", "core")
TP = ("yl", "x")
ALL = SEQ + TP
SCALING = 1.0 / math.sqrt(HEAD)
BF16 = jnp.bfloat16
F32 = jnp.float32


def position(group, groups):
    return group % (groups // 2) * 2 + group // (groups // 2)


def dot(a, b, ca, cb):
    return lax.dot_general(a, b, (((ca,), (cb,)), ((), ())), preferred_element_type=F32)


def project_kernel(text_ref, key_ref, value_ref, out_ref, states_ref, held_ref, arrived, here):
    groups = out_ref.shape[0]
    features = key_ref.shape[1]
    step = DT // CHUNKS
    states = pltpu.make_async_copy(text_ref, states_ref, here)
    states.start()
    copies = []
    for at in range(CHUNKS):
        rows = pl.ds(at * step, step)
        for which, ref in enumerate((key_ref, value_ref)):
            copy = pltpu.make_async_copy(ref.at[rows], held_ref.at[rows, pl.ds(which * features, features)], arrived.at[which, at])
            copy.start()
            copies.append(copy)
    states.wait()
    text = states_ref[...].reshape(-1, DT)
    wide = DT // groups
    for g in range(groups):
        first = position(g, groups) * wide
        out_ref[g, :, 2 * features :] = text[:, first : first + wide]
    total = None
    for at in range(CHUNKS):
        rows = slice(at * step, (at + 1) * step)
        copies[2 * at].wait()
        copies[2 * at + 1].wait()
        part = dot(text[:, rows], held_ref[rows], 1, 0)
        total = part if total is None else total + part
    total = total.astype(BF16)
    for g in range(groups):
        out_ref[g, :, : 2 * features] = total


def text_of(own_ref, other_ref, first_core, b, first):
    half = own_ref.shape[0] * 8
    own, other = [ref[:, b * 8 : (b + 1) * 8, first : first + HEAD].reshape(half, HEAD) for ref in (own_ref, other_ref)]
    return jnp.concatenate([jnp.where(first_core, own, other), jnp.where(first_core, other, own)], axis=0)


def score_kernel(lengths_ref, core_ref, query_ref, grad_ref, own_ref, other_ref, own_sum_ref, other_sum_ref, probs_ref, dscore_ref, columns_ref):
    samples, _, features = query_ref.shape
    groups = own_ref.shape[0]
    heads = features // HEAD
    first_core = core_ref[0] == 0
    half = groups * 8
    place = lax.broadcasted_iota(jnp.int32, (2 * half, 1), 0)
    within = place % half
    token = position(within // 8, groups) * 16 + (place // half) * 8 + within % 8
    columns_ref[0] = own_ref[:, :, 2 * features :]
    columns_ref[1] = other_ref[:, :, 2 * features :]

    def products(b, h):
        cols = slice(h * HEAD, (h + 1) * HEAD)
        key = text_of(own_ref, other_ref, first_core, b, h * HEAD)
        value = text_of(own_ref, other_ref, first_core, b, features + h * HEAD)
        return dot(key, query_ref[b, :, cols], 1, 1), dot(value, grad_ref[b, :, cols], 1, 1)

    def weigh(b, h, scores, dprob):
        scores = jnp.where(token < lengths_ref[b], scores, -1e30)
        weights = jnp.exp2((scores - jnp.max(scores, axis=0, keepdims=True)) * (SCALING * math.log2(math.e)))
        probs = weights * (1.0 / jnp.sum(weights, axis=0, keepdims=True))
        probs_low = probs.astype(BF16)
        delta = jnp.sum(probs * dprob, axis=0, keepdims=True)
        dscore = ((probs * SCALING) * (dprob - delta)).astype(BF16)
        probs_ref[b, h] = probs_low
        dscore_ref[b, h] = dscore
        return b, h, probs_low, dscore

    def add_up(b, h, probs_low, dscore):
        cols = slice(h * HEAD, (h + 1) * HEAD)
        key_sum = dot(dscore, query_ref[b, :, cols], 1, 0)
        value_sum = dot(probs_low, grad_ref[b, :, cols], 1, 0)
        own_sum = jnp.where(first_core, key_sum, value_sum)
        other_sum = jnp.where(first_core, value_sum, key_sum).astype(BF16)
        for side in range(2):
            at = slice(side * 16 + b * 8, side * 16 + (b + 1) * 8)
            from_side = slice(side * half, (side + 1) * half)
            own_sum_ref[:, at, cols] = own_sum[from_side].reshape(groups, 8, HEAD)
            other_sum_ref[:, at, cols] = other_sum[from_side].reshape(groups, 8, HEAD)

    jobs = [(b, h) for b in range(samples) for h in range(heads)]
    ahead = products(*jobs[0])
    behind = None
    for at, job in enumerate(jobs):
        now = ahead
        if at + 1 < len(jobs):
            ahead = products(*jobs[at + 1])
        if behind is not None:
            add_up(*behind)
        behind = weigh(*job, *now)
    add_up(*behind)


def attend_kernel(core_ref, own_ref, other_ref, probs_ref, dscore_ref, attended_ref, query_grad_ref, held_ref, sent):
    samples, heads = probs_ref.shape[:2]
    first_core = core_ref[0] == 0
    features = heads * HEAD
    copies = []
    for b in range(samples):
        for h in range(heads):
            cols = slice(h * HEAD, (h + 1) * HEAD)
            value = text_of(own_ref, other_ref, first_core, b, features + h * HEAD)
            held_ref[0, b, :, cols] = dot(probs_ref[b, h], value, 0, 0).astype(BF16)
            key = text_of(own_ref, other_ref, first_core, b, h * HEAD)
            held_ref[1, b, :, cols] = dot(dscore_ref[b, h], key, 0, 0).astype(BF16)
            part = pl.ds(h * HEAD, HEAD)
            for which, ref in enumerate((attended_ref, query_grad_ref)):
                copy = pltpu.make_async_copy(held_ref.at[which, b, :, part], ref.at[b, :, part], sent.at[which, b * heads + h])
                copy.start()
                copies.append(copy)
    for copy in copies:
        copy.wait()


def pair_sum_kernel(own_ref, other_ref, out_ref):
    out_ref[...] = (own_ref[...] + other_ref[...].astype(F32)).astype(BF16)


def total_kernel(parts_ref, out_ref):
    total = parts_ref[0].astype(F32)
    for g in range(1, parts_ref.shape[0]):
        total = total + parts_ref[g].astype(F32)
    total = total.astype(BF16)
    for g in range(out_ref.shape[0]):
        out_ref[g] = total


def weight_kernel(core_ref, columns_ref, total_ref, own_raw_ref, other_raw_ref, square_ref):
    groups, rows, features = total_ref.shape
    half = rows // 2
    core = core_ref[0]
    squares = None
    for raw_ref, feature_core in ((own_raw_ref, core), (other_raw_ref, 1 - core)):
        first = pl.multiple_of(feature_core * HEAD, HEAD)
        raw = None
        for which, side in ((0, core), (1, 1 - core)):
            text = columns_ref[which, :, :, pl.ds(first, HEAD)].reshape(groups * half, HEAD)
            total = total_ref[:, pl.ds(pl.multiple_of(side * half, half), half), :].reshape(groups * half, features)
            part = dot(text, total, 0, 0)
            raw = part if raw is None else raw + part
        raw_ref[...] = raw
        part = jnp.sum((raw * raw).reshape(-1, 8, features), axis=0)
        squares = part if squares is None else squares + part
    lanes = squares[:, :HEAD]
    for at in range(HEAD, features, HEAD):
        lanes = lanes + squares[:, at : at + HEAD]
    square_ref[...] = jnp.broadcast_to(jnp.sum(lanes, keepdims=True), square_ref.shape)


def scale_kernel(core_ref, own_ref, other_ref, squares_ref, key_ref, value_ref):
    overall = jnp.sum(squares_ref[...], keepdims=True)
    spread = jnp.sqrt(overall / (2.0 * DT * HEADS * HEAD) + 1e-06)
    factor = 1.0 / jnp.maximum(spread, 1.0)
    first_core = core_ref[0] == 0
    own = own_ref[...]
    other = other_ref[...]
    key_ref[...] = jnp.where(first_core, own, other) * factor
    value_ref[...] = jnp.where(first_core, other, own) * factor


def call(kernel, out, *args, scalars=0, far=0, far_out=False, scratch=(), mib=12):
    near, away = [pl.BlockSpec(memory_space=space) for space in (pltpu.VMEM, pl.ANY)]
    specs = [pl.BlockSpec(memory_space=pltpu.SMEM)] * scalars + [near] * (len(args) - scalars - far) + [away] * far
    out_spec = away if far_out else near
    return pl.pallas_call(
        kernel, out_shape=out, in_specs=specs, out_specs=out_spec if isinstance(out, jax.ShapeDtypeStruct) else [out_spec] * len(out),
        scratch_shapes=scratch, compiler_params=pltpu.CompilerParams(vmem_limit_bytes=int(mib * 1048576)),
    )(*args)


def shape(dims, dtype):
    return jax.ShapeDtypeStruct(dims, dtype)


def swap(array):
    return lax.ppermute(array, "core", [(0, 1), (1, 0)])


def exchange(array, axes):
    return lax.all_to_all(array, axes, 0, 0, tiled=True)


def per_device(video_query, text_states, key_weight, value_weight, text_lengths, output_grad):
    samples, video_rows, features = video_query.shape
    text_rows = samples * text_states.shape[1]
    groups = lax.axis_size(YZ)
    wide = 2 * features
    core = lax.axis_index("core").astype(jnp.int32).reshape(1)
    packed = call(
        project_kernel, shape((groups, text_rows, wide + DT // groups), BF16), text_states, key_weight, value_weight, far=3, mib=61,
        scratch=[
            pltpu.VMEM(text_states.shape, BF16), pltpu.VMEM((DT, wide), BF16),
            pltpu.SemaphoreType.DMA((2, CHUNKS)), pltpu.SemaphoreType.DMA,
        ],
    )
    own = exchange(packed, YZ)
    other = swap(own)
    like = shape(video_query.shape, BF16)
    block = (groups, 2 * text_rows, features)
    tall = shape((samples, features // HEAD, 2 * groups * 8, video_rows), BF16)
    own_sum, other_sum, probs, dscore, columns = call(
        score_kernel, [shape(block, F32), shape(block, BF16), tall, tall, shape((2, groups, text_rows, DT // groups), BF16)],
        text_lengths, core, video_query, output_grad, own, other, scalars=2,
    )
    attended, query_grad = call(
        attend_kernel, [like, like], core, own, other, probs, dscore, scalars=1, far_out=True,
        scratch=[pltpu.VMEM((2,) + video_query.shape, BF16), pltpu.SemaphoreType.DMA((2, samples * features // HEAD))],
    )
    pair = call(pair_sum_kernel, shape(block, BF16), own_sum, swap(other_sum))
    parts = exchange(pair, YZ)
    totals = exchange(call(total_kernel, shape(block, BF16), parts), YZ)
    every = lax.axis_size(ALL)
    weight = shape((HEAD, features), F32)
    own_raw, other_raw, squares = call(
        weight_kernel, [weight, weight, shape((every, 1), F32)], core, columns, totals, scalars=1,
    )
    squares = exchange(squares, ALL)
    key_weight_grad, value_weight_grad = call(
        scale_kernel, [weight, weight], core, own_raw, swap(other_raw), squares, scalars=1,
    )
    return attended, query_grad, key_weight_grad, value_weight_grad


def solution(mesh):
    split = Mesh(mesh.devices.reshape(8, 2, 2, 2, 4), ALL)
    return jax.shard_map(
        per_device,
        mesh=split,
        in_specs=(P(None, SEQ, TP), P(None, SEQ, None), P(None, TP), P(None, TP), P(), P(None, SEQ, TP)),
        out_specs=(P(None, SEQ, TP), P(None, SEQ, TP), P(SEQ, TP), P(SEQ, TP)),
        check_vma=False,
    )
```

```python
import math

import jax
import jax.numpy as jnp
from jax import lax
from jax.experimental import pallas as pl
from jax.experimental.pallas import tpu as pltpu
from jax.sharding import Mesh
from jax.sharding import PartitionSpec as P


DT = 4096
HEADS = 24
HEAD = 128
CHUNKS = 1
YZ = ("yh", "z")
SEQ = ("z", "yh", "core")
TP = ("yl", "x")
ALL = SEQ + TP
PEERS = ("core", "x", "yl", "yh", "z")
SCALING = 1.0 / math.sqrt(HEAD)
BF16 = jnp.bfloat16
F32 = jnp.float32


def position(group, groups):
    return group % (groups // 2) * 2 + group // (groups // 2)


def dot(a, b, ca, cb):
    return lax.dot_general(a, b, (((ca,), (cb,)), ((), ())), preferred_element_type=F32)


def project_kernel(text_ref, key_ref, value_ref, out_ref, states_ref, held_ref, arrived, here):
    groups = out_ref.shape[0]
    features = key_ref.shape[1]
    step = DT // CHUNKS
    states = pltpu.make_async_copy(text_ref, states_ref, here)
    states.start()
    copies = []
    for at in range(CHUNKS):
        rows = pl.ds(at * step, step)
        for which, ref in enumerate((key_ref, value_ref)):
            copy = pltpu.make_async_copy(ref.at[rows], held_ref.at[rows, pl.ds(which * features, features)], arrived.at[which, at])
            copy.start()
            copies.append(copy)
    states.wait()
    text = states_ref[...].reshape(-1, DT)
    wide = DT // groups
    for g in range(groups):
        first = position(g, groups) * wide
        out_ref[g, :, 2 * features :] = text[:, first : first + wide]
    total = None
    for at in range(CHUNKS):
        rows = slice(at * step, (at + 1) * step)
        copies[2 * at].wait()
        copies[2 * at + 1].wait()
        part = dot(text[:, rows], held_ref[rows], 1, 0)
        total = part if total is None else total + part
    total = total.astype(BF16)
    for g in range(groups):
        out_ref[g, :, : 2 * features] = total


def text_of(own_ref, other_ref, first_core, b, first):
    half = own_ref.shape[0] * 8
    own, other = [ref[:, b * 8 : (b + 1) * 8, first : first + HEAD].reshape(half, HEAD) for ref in (own_ref, other_ref)]
    return jnp.concatenate([jnp.where(first_core, own, other), jnp.where(first_core, other, own)], axis=0)


def score_kernel(lengths_ref, core_ref, query_ref, grad_ref, own_ref, other_ref, own_sum_ref, other_sum_ref, probs_ref, dscore_ref, columns_ref):
    samples, _, features = query_ref.shape
    groups = own_ref.shape[0]
    heads = features // HEAD
    first_core = core_ref[0] == 0
    half = groups * 8
    place = lax.broadcasted_iota(jnp.int32, (2 * half, 1), 0)
    within = place % half
    token = position(within // 8, groups) * 16 + (place // half) * 8 + within % 8
    columns_ref[0] = own_ref[:, :, 2 * features :]
    columns_ref[1] = other_ref[:, :, 2 * features :]

    def products(b, h):
        cols = slice(h * HEAD, (h + 1) * HEAD)
        key = text_of(own_ref, other_ref, first_core, b, h * HEAD)
        value = text_of(own_ref, other_ref, first_core, b, features + h * HEAD)
        return dot(key, query_ref[b, :, cols], 1, 1), dot(value, grad_ref[b, :, cols], 1, 1)

    def weigh(b, h, scores, dprob):
        scores = jnp.where(token < lengths_ref[b], scores, -1e30)
        weights = jnp.exp2((scores - jnp.max(scores, axis=0, keepdims=True)) * (SCALING * math.log2(math.e)))
        probs = weights * (1.0 / jnp.sum(weights, axis=0, keepdims=True))
        probs_low = probs.astype(BF16)
        delta = jnp.sum(probs * dprob, axis=0, keepdims=True)
        dscore = ((probs * SCALING) * (dprob - delta)).astype(BF16)
        probs_ref[b, h] = probs_low
        dscore_ref[b, h] = dscore
        return b, h, probs_low, dscore

    def add_up(b, h, probs_low, dscore):
        cols = slice(h * HEAD, (h + 1) * HEAD)
        key_sum = dot(dscore, query_ref[b, :, cols], 1, 0)
        value_sum = dot(probs_low, grad_ref[b, :, cols], 1, 0)
        own_sum = jnp.where(first_core, key_sum, value_sum)
        other_sum = jnp.where(first_core, value_sum, key_sum).astype(BF16)
        for side in range(2):
            at = slice(side * 16 + b * 8, side * 16 + (b + 1) * 8)
            from_side = slice(side * half, (side + 1) * half)
            own_sum_ref[:, at, cols] = own_sum[from_side].reshape(groups, 8, HEAD)
            other_sum_ref[:, at, cols] = other_sum[from_side].reshape(groups, 8, HEAD)

    jobs = [(b, h) for b in range(samples) for h in range(heads)]
    ahead = products(*jobs[0])
    behind = None
    for at, job in enumerate(jobs):
        now = ahead
        if at + 1 < len(jobs):
            ahead = products(*jobs[at + 1])
        if behind is not None:
            add_up(*behind)
        behind = weigh(*job, *now)
    add_up(*behind)


def attend_kernel(core_ref, own_ref, other_ref, probs_ref, dscore_ref, attended_ref, query_grad_ref, held_ref, sent):
    samples, heads = probs_ref.shape[:2]
    first_core = core_ref[0] == 0
    features = heads * HEAD
    copies = []
    for b in range(samples):
        for h in range(heads):
            cols = slice(h * HEAD, (h + 1) * HEAD)
            value = text_of(own_ref, other_ref, first_core, b, features + h * HEAD)
            held_ref[0, b, :, cols] = dot(probs_ref[b, h], value, 0, 0).astype(BF16)
            key = text_of(own_ref, other_ref, first_core, b, h * HEAD)
            held_ref[1, b, :, cols] = dot(dscore_ref[b, h], key, 0, 0).astype(BF16)
            part = pl.ds(h * HEAD, HEAD)
            for which, ref in enumerate((attended_ref, query_grad_ref)):
                copy = pltpu.make_async_copy(held_ref.at[which, b, :, part], ref.at[b, :, part], sent.at[which, b * heads + h])
                copy.start()
                copies.append(copy)
    for copy in copies:
        copy.wait()


def pair_sum_kernel(own_ref, other_ref, out_ref):
    out_ref[...] = (own_ref[...] + other_ref[...].astype(F32)).astype(BF16)


def total_kernel(parts_ref, out_ref):
    total = parts_ref[0].astype(F32)
    for g in range(1, parts_ref.shape[0]):
        total = total + parts_ref[g].astype(F32)
    total = total.astype(BF16)
    for g in range(out_ref.shape[0]):
        out_ref[g] = total


def weight_kernel(core_ref, columns_ref, total_ref, own_raw_ref, other_raw_ref, square_ref):
    groups, rows, features = total_ref.shape
    half = rows // 2
    core = core_ref[0]
    squares = None
    for raw_ref, feature_core in ((own_raw_ref, core), (other_raw_ref, 1 - core)):
        first = pl.multiple_of(feature_core * HEAD, HEAD)
        raw = None
        for which, side in ((0, core), (1, 1 - core)):
            text = columns_ref[which, :, :, pl.ds(first, HEAD)].reshape(groups * half, HEAD)
            total = total_ref[:, pl.ds(pl.multiple_of(side * half, half), half), :].reshape(groups * half, features)
            part = dot(text, total, 0, 0)
            raw = part if raw is None else raw + part
        raw_ref[...] = raw
        part = jnp.sum((raw * raw).reshape(-1, 8, features), axis=0)
        squares = part if squares is None else squares + part
    lanes = squares[:, :HEAD]
    for at in range(HEAD, features, HEAD):
        lanes = lanes + squares[:, at : at + HEAD]
    square_ref[...] = jnp.broadcast_to(jnp.sum(lanes, keepdims=True), square_ref.shape)


def scale_kernel(core_ref, own_ref, other_ref, squares_ref, key_ref, value_ref):
    overall = jnp.sum(squares_ref[...], keepdims=True)
    spread = jnp.sqrt(overall / (2.0 * DT * HEADS * HEAD) + 1e-06)
    factor = 1.0 / jnp.maximum(spread, 1.0)
    first_core = core_ref[0] == 0
    own = own_ref[...]
    other = other_ref[...]
    key_ref[...] = jnp.where(first_core, own, other) * factor
    value_ref[...] = jnp.where(first_core, other, own) * factor


def call(kernel, out, *args, scalars=0, far=0, far_out=False, scratch=(), mib=12):
    near, away = [pl.BlockSpec(memory_space=space) for space in (pltpu.VMEM, pl.ANY)]
    specs = [pl.BlockSpec(memory_space=pltpu.SMEM)] * scalars + [near] * (len(args) - scalars - far) + [away] * far
    out_spec = away if far_out else near
    return pl.pallas_call(
        kernel, out_shape=out, in_specs=specs, out_specs=out_spec if isinstance(out, jax.ShapeDtypeStruct) else [out_spec] * len(out),
        scratch_shapes=scratch, compiler_params=pltpu.CompilerParams(vmem_limit_bytes=int(mib * 1048576)),
    )(*args)


def shape(dims, dtype):
    return jax.ShapeDtypeStruct(dims, dtype)


def swap(array):
    return lax.ppermute(array, "core", [(0, 1), (1, 0)])


def exchange(array, axes):
    return lax.all_to_all(array, axes, 0, 0, tiled=True)


def per_device(video_query, text_states, key_weight, value_weight, text_lengths, output_grad):
    samples, video_rows, features = video_query.shape
    text_rows = samples * text_states.shape[1]
    groups = lax.axis_size(YZ)
    wide = 2 * features
    core = lax.axis_index("core").astype(jnp.int32).reshape(1)
    packed = call(
        project_kernel, shape((groups, text_rows, wide + DT // groups), BF16), text_states, key_weight, value_weight, far=3, mib=61,
        scratch=[
            pltpu.VMEM(text_states.shape, BF16), pltpu.VMEM((DT, wide), BF16),
            pltpu.SemaphoreType.DMA((2, CHUNKS)), pltpu.SemaphoreType.DMA,
        ],
    )
    own = exchange(packed, YZ)
    other = swap(own)
    like = shape(video_query.shape, BF16)
    block = (groups, 2 * text_rows, features)
    tall = shape((samples, features // HEAD, 2 * groups * 8, video_rows), BF16)
    own_sum, other_sum, probs, dscore, columns = call(
        score_kernel, [shape(block, F32), shape(block, BF16), tall, tall, shape((2, groups, text_rows, DT // groups), BF16)],
        text_lengths, core, video_query, output_grad, own, other, scalars=2,
    )
    attended, query_grad = call(
        attend_kernel, [like, like], core, own, other, probs, dscore, scalars=1, far_out=True,
        scratch=[pltpu.VMEM((2,) + video_query.shape, BF16), pltpu.SemaphoreType.DMA((2, samples * features // HEAD))],
    )
    pair = call(pair_sum_kernel, shape(block, BF16), own_sum, swap(other_sum))
    parts = exchange(pair, YZ)
    totals = exchange(call(total_kernel, shape(block, BF16), parts), YZ)
    every = lax.axis_size(ALL)
    weight = shape((HEAD, features), F32)
    own_raw, other_raw, squares = call(
        weight_kernel, [weight, weight, shape((every, 1), F32)], core, columns, totals, scalars=1,
    )
    squares = exchange(squares, PEERS)
    key_weight_grad, value_weight_grad = call(
        scale_kernel, [weight, weight], core, own_raw, swap(other_raw), squares, scalars=1,
    )
    return attended, query_grad, key_weight_grad, value_weight_grad


def solution(mesh):
    split = Mesh(mesh.devices.reshape(8, 2, 2, 2, 4), ALL)
    return jax.shard_map(
        per_device,
        mesh=split,
        in_specs=(P(None, SEQ, TP), P(None, SEQ, None), P(None, TP), P(None, TP), P(), P(None, SEQ, TP)),
        out_specs=(P(None, SEQ, TP), P(None, SEQ, TP), P(SEQ, TP), P(SEQ, TP)),
        check_vma=False,
    )
```

```python
import math

import jax
import jax.numpy as jnp
from jax import lax
from jax.experimental import pallas as pl
from jax.experimental.pallas import tpu as pltpu
from jax.sharding import Mesh
from jax.sharding import PartitionSpec as P


DT = 4096
HEADS = 24
HEAD = 128
CHUNKS = 2
YZ = ("yh", "z")
SEQ = ("z", "yh", "core")
TP = ("yl", "x")
ALL = SEQ + TP
SCALING = 1.0 / math.sqrt(HEAD)
BF16 = jnp.bfloat16
F32 = jnp.float32


def position(group, groups):
    return group % (groups // 2) * 2 + group // (groups // 2)


def dot(a, b, ca, cb):
    return lax.dot_general(a, b, (((ca,), (cb,)), ((), ())), preferred_element_type=F32)


def project_kernel(text_ref, key_ref, value_ref, out_ref, states_ref, held_ref, arrived, here):
    groups = out_ref.shape[0]
    features = key_ref.shape[1]
    step = DT // CHUNKS
    states = pltpu.make_async_copy(text_ref, states_ref, here)
    states.start()
    copies = []
    for at in range(CHUNKS):
        rows = pl.ds(at * step, step)
        for which, ref in enumerate((key_ref, value_ref)):
            copy = pltpu.make_async_copy(ref.at[rows], held_ref.at[rows, pl.ds(which * features, features)], arrived.at[which, at])
            copy.start()
            copies.append(copy)
    states.wait()
    text = states_ref[...].reshape(-1, DT)
    wide = DT // groups
    for g in range(groups):
        first = position(g, groups) * wide
        out_ref[g, :, 2 * features :] = text[:, first : first + wide]
    total = None
    for at in range(CHUNKS):
        rows = slice(at * step, (at + 1) * step)
        copies[2 * at].wait()
        copies[2 * at + 1].wait()
        part = dot(text[:, rows], held_ref[rows], 1, 0)
        total = part if total is None else total + part
    total = total.astype(BF16)
    for g in range(groups):
        out_ref[g, :, : 2 * features] = total


def text_of(own_ref, other_ref, first_core, b, first):
    half = own_ref.shape[0] * 8
    own, other = [ref[:, b * 8 : (b + 1) * 8, first : first + HEAD].reshape(half, HEAD) for ref in (own_ref, other_ref)]
    return jnp.concatenate([jnp.where(first_core, own, other), jnp.where(first_core, other, own)], axis=0)


def score_kernel(lengths_ref, core_ref, query_ref, grad_ref, own_ref, other_ref, own_sum_ref, other_sum_ref, probs_ref, dscore_ref, columns_ref):
    samples, _, features = query_ref.shape
    groups = own_ref.shape[0]
    heads = features // HEAD
    first_core = core_ref[0] == 0
    half = groups * 8
    place = lax.broadcasted_iota(jnp.int32, (2 * half, 1), 0)
    within = place % half
    token = position(within // 8, groups) * 16 + (place // half) * 8 + within % 8
    columns_ref[0] = own_ref[:, :, 2 * features :]
    columns_ref[1] = other_ref[:, :, 2 * features :]

    def products(b, h):
        cols = slice(h * HEAD, (h + 1) * HEAD)
        key = text_of(own_ref, other_ref, first_core, b, h * HEAD)
        value = text_of(own_ref, other_ref, first_core, b, features + h * HEAD)
        return dot(key, query_ref[b, :, cols], 1, 1), dot(value, grad_ref[b, :, cols], 1, 1)

    def weigh(b, h, scores, dprob):
        scores = jnp.where(token < lengths_ref[b], scores, -1e30)
        weights = jnp.exp2((scores - jnp.max(scores, axis=0, keepdims=True)) * (SCALING * math.log2(math.e)))
        inverse = 1.0 / jnp.sum(weights, axis=0, keepdims=True)
        probs = weights * inverse
        probs_low = probs.astype(BF16)
        delta = jnp.sum(weights * dprob, axis=0, keepdims=True) * inverse
        dscore = ((probs * SCALING) * (dprob - delta)).astype(BF16)
        probs_ref[b, h] = probs_low
        dscore_ref[b, h] = dscore
        return b, h, probs_low, dscore

    def add_up(b, h, probs_low, dscore):
        cols = slice(h * HEAD, (h + 1) * HEAD)
        key_sum = dot(dscore, query_ref[b, :, cols], 1, 0)
        value_sum = dot(probs_low, grad_ref[b, :, cols], 1, 0)
        own_sum = jnp.where(first_core, key_sum, value_sum)
        other_sum = jnp.where(first_core, value_sum, key_sum).astype(BF16)
        for side in range(2):
            at = slice(side * 16 + b * 8, side * 16 + (b + 1) * 8)
            from_side = slice(side * half, (side + 1) * half)
            own_sum_ref[:, at, cols] = own_sum[from_side].reshape(groups, 8, HEAD)
            other_sum_ref[:, at, cols] = other_sum[from_side].reshape(groups, 8, HEAD)

    jobs = [(b, h) for b in range(samples) for h in range(heads)]
    ahead = products(*jobs[0])
    behind = None
    for at, job in enumerate(jobs):
        now = ahead
        if at + 1 < len(jobs):
            ahead = products(*jobs[at + 1])
        if behind is not None:
            add_up(*behind)
        behind = weigh(*job, *now)
    add_up(*behind)


def attend_kernel(core_ref, own_ref, other_ref, probs_ref, dscore_ref, attended_ref, query_grad_ref, held_ref, sent):
    samples, heads = probs_ref.shape[:2]
    first_core = core_ref[0] == 0
    features = heads * HEAD
    copies = []
    for b in range(samples):
        for h in range(heads):
            cols = slice(h * HEAD, (h + 1) * HEAD)
            value = text_of(own_ref, other_ref, first_core, b, features + h * HEAD)
            held_ref[0, b, :, cols] = dot(probs_ref[b, h], value, 0, 0).astype(BF16)
            key = text_of(own_ref, other_ref, first_core, b, h * HEAD)
            held_ref[1, b, :, cols] = dot(dscore_ref[b, h], key, 0, 0).astype(BF16)
            part = pl.ds(h * HEAD, HEAD)
            for which, ref in enumerate((attended_ref, query_grad_ref)):
                copy = pltpu.make_async_copy(held_ref.at[which, b, :, part], ref.at[b, :, part], sent.at[which, b * heads + h])
                copy.start()
                copies.append(copy)
    for copy in copies:
        copy.wait()


def pair_sum_kernel(own_ref, other_ref, out_ref):
    out_ref[...] = (own_ref[...] + other_ref[...].astype(F32)).astype(BF16)


def total_kernel(parts_ref, out_ref):
    total = parts_ref[0].astype(F32)
    for g in range(1, parts_ref.shape[0]):
        total = total + parts_ref[g].astype(F32)
    total = total.astype(BF16)
    for g in range(out_ref.shape[0]):
        out_ref[g] = total


def weight_kernel(core_ref, columns_ref, total_ref, own_raw_ref, other_raw_ref, square_ref):
    groups, rows, features = total_ref.shape
    half = rows // 2
    core = core_ref[0]
    squares = None
    for raw_ref, feature_core in ((own_raw_ref, core), (other_raw_ref, 1 - core)):
        first = pl.multiple_of(feature_core * HEAD, HEAD)
        raw = None
        for which, side in ((0, core), (1, 1 - core)):
            text = columns_ref[which, :, :, pl.ds(first, HEAD)].reshape(groups * half, HEAD)
            total = total_ref[:, pl.ds(pl.multiple_of(side * half, half), half), :].reshape(groups * half, features)
            part = dot(text, total, 0, 0)
            raw = part if raw is None else raw + part
        raw_ref[...] = raw
        part = jnp.sum((raw * raw).reshape(-1, 8, features), axis=0)
        squares = part if squares is None else squares + part
    lanes = squares[:, :HEAD]
    for at in range(HEAD, features, HEAD):
        lanes = lanes + squares[:, at : at + HEAD]
    square_ref[...] = jnp.broadcast_to(jnp.sum(lanes, keepdims=True), square_ref.shape)


def scale_kernel(core_ref, own_ref, other_ref, squares_ref, key_ref, value_ref):
    overall = jnp.sum(squares_ref[...], keepdims=True)
    spread = jnp.sqrt(overall / (2.0 * DT * HEADS * HEAD) + 1e-06)
    factor = 1.0 / jnp.maximum(spread, 1.0)
    first_core = core_ref[0] == 0
    own = own_ref[...]
    other = other_ref[...]
    key_ref[...] = jnp.where(first_core, own, other) * factor
    value_ref[...] = jnp.where(first_core, other, own) * factor


def call(kernel, out, *args, scalars=0, far=0, far_out=False, scratch=(), mib=12):
    near, away = [pl.BlockSpec(memory_space=space) for space in (pltpu.VMEM, pl.ANY)]
    specs = [pl.BlockSpec(memory_space=pltpu.SMEM)] * scalars + [near] * (len(args) - scalars - far) + [away] * far
    out_spec = away if far_out else near
    return pl.pallas_call(
        kernel, out_shape=out, in_specs=specs, out_specs=out_spec if isinstance(out, jax.ShapeDtypeStruct) else [out_spec] * len(out),
        scratch_shapes=scratch, compiler_params=pltpu.CompilerParams(vmem_limit_bytes=int(mib * 1048576)),
    )(*args)


def shape(dims, dtype):
    return jax.ShapeDtypeStruct(dims, dtype)


def swap(array):
    return lax.ppermute(array, "core", [(0, 1), (1, 0)])


def exchange(array, axes):
    return lax.all_to_all(array, axes, 0, 0, tiled=True)


def per_device(video_query, text_states, key_weight, value_weight, text_lengths, output_grad):
    samples, video_rows, features = video_query.shape
    text_rows = samples * text_states.shape[1]
    groups = lax.axis_size(YZ)
    wide = 2 * features
    core = lax.axis_index("core").astype(jnp.int32).reshape(1)
    packed = call(
        project_kernel, shape((groups, text_rows, wide + DT // groups), BF16), text_states, key_weight, value_weight, far=3, mib=61,
        scratch=[
            pltpu.VMEM(text_states.shape, BF16), pltpu.VMEM((DT, wide), BF16),
            pltpu.SemaphoreType.DMA((2, CHUNKS)), pltpu.SemaphoreType.DMA,
        ],
    )
    own = exchange(packed, YZ)
    other = swap(own)
    like = shape(video_query.shape, BF16)
    block = (groups, 2 * text_rows, features)
    tall = shape((samples, features // HEAD, 2 * groups * 8, video_rows), BF16)
    own_sum, other_sum, probs, dscore, columns = call(
        score_kernel, [shape(block, F32), shape(block, BF16), tall, tall, shape((2, groups, text_rows, DT // groups), BF16)],
        text_lengths, core, video_query, output_grad, own, other, scalars=2,
    )
    attended, query_grad = call(
        attend_kernel, [like, like], core, own, other, probs, dscore, scalars=1, far_out=True,
        scratch=[pltpu.VMEM((2,) + video_query.shape, BF16), pltpu.SemaphoreType.DMA((2, samples * features // HEAD))],
    )
    pair = call(pair_sum_kernel, shape(block, BF16), own_sum, swap(other_sum))
    parts = exchange(pair, YZ)
    totals = exchange(call(total_kernel, shape(block, BF16), parts), YZ)
    every = lax.axis_size(ALL)
    weight = shape((HEAD, features), F32)
    own_raw, other_raw, squares = call(
        weight_kernel, [weight, weight, shape((every, 1), F32)], core, columns, totals, scalars=1,
    )
    squares = exchange(squares, ALL)
    key_weight_grad, value_weight_grad = call(
        scale_kernel, [weight, weight], core, own_raw, swap(other_raw), squares, scalars=1,
    )
    return attended, query_grad, key_weight_grad, value_weight_grad


def solution(mesh):
    split = Mesh(mesh.devices.reshape(8, 2, 2, 2, 4), ALL)
    return jax.shard_map(
        per_device,
        mesh=split,
        in_specs=(P(None, SEQ, TP), P(None, SEQ, None), P(None, TP), P(None, TP), P(), P(None, SEQ, TP)),
        out_specs=(P(None, SEQ, TP), P(None, SEQ, TP), P(SEQ, TP), P(SEQ, TP)),
        check_vma=False,
    )
```
